128 devices in a mesh: dp: 8 (over x, z_hi), cls: 16 (over z_lo, y, core).
Axes of the slice: x: 4, y: 4, z: 4 (z_hi: 2, z_lo: 2; z = z_hi * 2 + z_lo), core: 2. Of those that a mesh axis runs over, the one named last changes fastest.
Arguments:
- sketches: bfloat16 [32768, 4096], P(('dp', 'cls')), may hold values from -6 to 6
- labels: int32 [32768], P(('dp', 'cls')), may hold values from 0 to 15, as said below
- places: int32 [32768], P(('dp', 'cls')), may hold values from 0 to 4095, as said below
- counts: int32 [16, 8, 128], P('cls'), may hold values from 0 to 4, as said below
- chosen: int32 [3, 16], P(None, 'cls'), may hold values from 0 to 4095, as said below
Outputs:
- gain_scores: float32 [3, 16, 4096], P(None, 'cls', 'dp')
- coverage: float32 [16, 4096], P('cls', 'dp')
The draws below stay inside these ranges and needn't reach their ends.
Inputs may be any that keep to these rules, and one draw needn't show every extreme that they name: `labels`: every class has 8 or more examples. `places`: an example of device s (its index along dp and cls together) with class k has place m * 512 + s * 4 + j in class k's block: m is the member of dp that receives it, and for each k, m and s the j run over 0 to counts[k, m, s] - 1 without gaps, so no two examples share a place. In every draw one class and member receive 4 examples from every device. counts[k, m, s] is the number of examples of device s that take places of class k on member m. chosen[t, k] is a place of class k's block that holds an example; the 3 picks of a class differ.
All inputs are finite; a program needn't handle non-finite values.
Results may differ from the reference program's by a relative error of at most 0.0003.
Values may be sent and summed in bfloat16 or wider, within the bound.
No kernel may reach another device: no remote copies, remote signals or barrier semaphores. Data moves between devices by JAX's collectives and lax.ppermute only.
A program may use at most 128 MiB of HBM per device.

```python
import jax
import jax.numpy as jnp
from jax import lax

D = 4096
ROW_DEV = 256
STEPS = 3
CLASSES = 16
SUB = 4
CAP = 512
BLOCK = 4096
ROWS = 32768
N_DP = 8
DEVICES = 128


def layout_tables(key):
    slot_count = 2 * ROW_DEV
    class_key, full_key, member_key, base_key, pick_key = jax.random.split(jax.random.fold_in(key, 7), 5)
    class_level = jax.random.randint(class_key, (CLASSES,), 0, 3)
    full_class = jax.random.randint(full_key, (), 0, CLASSES)
    full_member = jax.random.randint(member_key, (), 0, N_DP)
    item_index = jnp.arange(slot_count, dtype=jnp.int32)
    item_member = item_index // (CLASSES * SUB)
    item_class = item_index // SUB % CLASSES
    item_place = item_index % SUB
    source = jnp.arange(DEVICES, dtype=jnp.int32)[:, None]
    promised = (item_class[None, :] == source % CLASSES) & (item_member[None, :] == source // CLASSES % N_DP) & (item_place[None, :] == 0)
    full_item = (item_class == full_class) & (item_member == full_member)
    base = jax.random.randint(base_key, (DEVICES, slot_count), 0, 2 ** 16)
    level = base + class_level[item_class][None, :] * 2 ** 16 + promised.astype(jnp.int32) * 2 ** 18 + full_item.astype(jnp.int32)[None, :] * 2 ** 19
    score = level * slot_count + item_index[None, :]
    top_scores, picked_items = lax.top_k(score, ROW_DEV)
    group = picked_items // SUB
    same_group = group[:, :, None] == group[:, None, :]
    earlier = picked_items[:, None, :] < picked_items[:, :, None]
    rank = jnp.sum((same_group & earlier).astype(jnp.int32), axis=2)
    member = group // CLASSES
    klass = group % CLASSES
    places = member * CAP + source * SUB + rank
    group_hits = (group[:, :, None] == jnp.arange(N_DP * CLASSES, dtype=jnp.int32)[None, None, :]).astype(jnp.int32)
    per_group = jnp.sum(group_hits, axis=1).reshape(DEVICES, N_DP, CLASSES)
    counts = jnp.transpose(per_group, (2, 1, 0))
    valid = (jnp.arange(SUB, dtype=jnp.int32)[None, None, None, :] < counts[:, :, :, None]).reshape(CLASSES, BLOCK)
    noise = jax.random.randint(pick_key, (CLASSES, BLOCK), 0, 256)
    pick_score = (noise + valid.astype(jnp.int32) * 512) * BLOCK + jnp.arange(BLOCK, dtype=jnp.int32)[None, :]
    top_picks, pick_places = lax.top_k(pick_score, STEPS)
    return (klass.reshape(-1), places.reshape(-1), counts, jnp.transpose(pick_places))


def draw_labels(key, part):
    return layout_tables(key)[0].astype(jnp.int32)


def draw_places(key, part):
    return layout_tables(key)[1].astype(jnp.int32)


def draw_counts(key, part):
    return layout_tables(key)[2].astype(jnp.int32)


def draw_chosen(key, part):
    return layout_tables(key)[3].astype(jnp.int32)


def draw_sketches(key, part):
    labels = layout_tables(key)[0].astype(jnp.int32)
    mean_key, noise_key, scale_key = jax.random.split(jax.random.fold_in(key, 11), 3)
    class_means = jnp.clip(jax.random.normal(mean_key, (CLASSES, D), jnp.float32), -4.2, 4.2)
    centers = 0.6 * class_means[labels]
    noise = jnp.clip(jax.random.normal(noise_key, (ROWS, D), jnp.float32), -4.2, 4.2)
    raw = centers + noise
    row_rms = jnp.sqrt(jnp.mean(raw * raw, axis=1, keepdims=True))
    scale = jnp.exp(jax.random.uniform(scale_key, (ROWS, 1), jnp.float32, jnp.log(0.98), jnp.log(1.02)))
    values = jnp.clip(scale * raw / row_rms, -6.0, 6.0)
    return values.astype(jnp.bfloat16)


def setup_inputs(seed: int = 0) -> dict:
    seeds = jax.random.split(jax.random.key(seed), 6)
    sketches = draw_sketches(jax.random.fold_in(seeds[5], 71), 0)
    labels = draw_labels(jax.random.fold_in(seeds[5], 71), 0)
    places = draw_places(jax.random.fold_in(seeds[5], 71), 0)
    counts = draw_counts(jax.random.fold_in(seeds[5], 71), 0)
    chosen = draw_chosen(jax.random.fold_in(seeds[5], 71), 0)
    return {"sketches": sketches, "labels": labels, "places": places, "counts": counts, "chosen": chosen}


def class_scores(class_block, class_counts, class_picks):
    wide = class_block.astype(jnp.float32)
    norms = jnp.sum(wide * wide, axis=1)
    inner = jnp.dot(class_block, class_block.T, preferred_element_type=jnp.float32)
    spread = (norms[:, None] + norms[None, :] - 2.0 * inner) / D
    valid = (jnp.arange(SUB, dtype=jnp.int32)[None, None, :] < class_counts[:, :, None]).reshape(-1)
    weight = valid.astype(jnp.float32)
    bound = jnp.max(jnp.where(valid[:, None] & valid[None, :], spread, 0.0))
    similar = bound - spread
    total = jnp.sum(class_counts).astype(jnp.float32)
    cover = jnp.zeros((similar.shape[0],), jnp.float32)
    scores = []
    for turn_index in range(STEPS):
        scores.append(jnp.sum(weight[:, None] * jnp.maximum(similar - cover[:, None], 0.0), axis=0) * weight / total)
        column = lax.dynamic_index_in_dim(similar, class_picks[turn_index].astype(jnp.int32), 1, keepdims=False)
        cover = jnp.maximum(cover, column)
    return jnp.stack(scores), cover * weight


def score_item(packed):
    return class_scores(packed[0], packed[1], packed[2])


def reference(sketches, labels, places, counts, chosen):
    flat_index = (labels * BLOCK + places).astype(jnp.int32)
    blocks = jnp.zeros((CLASSES * BLOCK, D), sketches.dtype).at[flat_index].set(sketches)
    blocks = blocks.reshape(CLASSES, BLOCK, D)
    scores, cover = lax.map(score_item, (blocks, counts, jnp.transpose(chosen)))
    return jnp.transpose(scores, (1, 0, 2)), cover
```

```python
import jax
import jax.numpy as jnp
from jax import lax
from jax.sharding import PartitionSpec as P

AX = ("dp", "cls")
F32 = jnp.float32
BF16 = jnp.bfloat16
BIG = 1e30
CHUNKS = (5, 5, 4, 2)


def dix(x, y, z, c):
    return x * 32 + (z // 2) * 16 + (z % 2) * 8 + y * 2 + c


def xyz(d):
    return d // 32, (d // 2) % 4, ((d // 16) % 2) * 2 + (d // 8) % 2, d % 2


DEV = range(128)
MATE = ((1, 0, 3, 2), (3, 2, 1, 0))
PAIRS = (((0, 1), (2, 3)), ((2, 1), (0, 3)))


def mate(d):
    x, y, z, c = xyz(d)
    return dix(x, MATE[c][y], z, c)


def along(d, k):
    x, y, z, c = xyz(d)
    return dix((x + k) % 4, y, z, c) if c == 0 else dix(x, y, (z + k) % 4, c)


def side(d):
    return xyz(d)[1] % 2


SWAP = [(d, d ^ 1) for d in DEV]
UP = [(d, along(d, 1)) for d in DEV]
DOWN = [(d, along(d, -1)) for d in DEV]
ACROSS = [(d, mate(d)) for d in DEV]
FOURTH = [(d, mate(d) if side(d) == 1 else mate(along(d, 1))) for d in DEV]


def regroup_groups():
    groups = []
    for x in range(4):
        for ys in ((0, 3), (1, 2)):
            groups.append([dix(x, y, z, 0) for y in ys for z in range(4)])
    for z in range(4):
        for ys in ((1, 0), (2, 3)):
            groups.append([dix(x, y, z, 1) for y in ys for x in range(4)])
    return groups


def class_groups():
    groups = []
    for c in (0, 1):
        for pair in PAIRS[c]:
            for u in range(4):
                group = [dix(t, y, u, 0) if c == 0 else dix(u, y, t, 1) for t in range(4) for y in pair]
                groups.append(group)
    return groups


def final_groups():
    groups = []
    for c in (0, 1):
        for pair in PAIRS[c]:
            groups.append([dix(x, y, z, c) for x in range(4) for z in range(4) for y in pair])
    return groups


def info_pairs():
    out = []
    for d in DEV:
        x, y, z, c = xyz(d)
        zh, zl = z // 2, z % 2
        if c == 0:
            src = dix(x, (y // 2) * 2 + zh, (y % 2) * 2 + zl, 0)
        else:
            yk = y if y % 2 == x % 2 else MATE[1][y]
            src = dix(zh * 2 + zl, yk, (y % 2) * 2 + x // 2, 1)
        out.append((src, d))
    return out


INFO = info_pairs()


def send(value, pairs):
    return lax.ppermute(value, AX, pairs)


def iota(shape, dim):
    return lax.broadcasted_iota(jnp.int32, shape, dim)


def inner(left, right):
    return lax.dot_general(left, right, (((1,), (1,)), ((), ())), preferred_element_type=F32)


def exact(left, right):
    return jnp.dot(left, right, precision=lax.Precision.HIGHEST, preferred_element_type=F32)


def reach(pair, rows, columns):
    out = [jnp.sum(pair, axis=0)]
    for t in (2, 3):
        out.append(jnp.sum(jnp.maximum(pair + rows[t][:, None] - columns[0][None, :], 0.0), axis=0))
    return jnp.stack(out)


def furthest(pair, rows, columns):
    return jnp.max(rows[1][:, None] + columns[1][None, :] - pair)


def source_of(place_in_line, x, z, y, core, row):
    group, sub, member, slot = row // 64, row // 32 % 2, row // 4 % 8, row % 4
    i, w = group // 4, group % 4
    outer = (y == 0) | (y == 3)
    low = y < 2
    y0 = jnp.where(outer, 3 * i, 1 + i)
    y1 = jnp.where(low, 1 - i, 2 + i)
    sx = jnp.where(core == 0, x, w)
    sz = jnp.where(core == 0, w, z)
    sy = jnp.where(core == 0, y0, y1)
    return dix(sx, sy, sz, jnp.where(sub == 0, 0, 1)), member, slot


def body(sketches, labels, places, counts, chosen):
    rows_dev, width = sketches.shape
    dp, cls = lax.axis_index("dp"), lax.axis_index("cls")
    x, zh, zl, y, core = dp // 2, dp % 2, cls // 8, cls // 2 % 4, cls % 2
    z = zh * 2 + zl
    edge = y % 2
    first = core == 0

    packed = jnp.concatenate([counts[0], jnp.broadcast_to(chosen, (3, 128))], axis=0)
    packed = send(packed, INFO)
    host_counts = packed[:8].astype(F32)
    picks = packed[8:11, 0]

    k_core, k_y, k_zl = labels % 2, labels // 2 % 4, labels // 8
    group = jnp.where(
        k_core == 0,
        (k_y // 2) * 4 + (k_y % 2) * 2 + k_zl,
        ((k_y + 3) % 4 // 2) * 4 + k_zl * 2 + k_y % 2,
    )
    spot = group * 64 + core * 32 + places // 512 * 4 + places % 4
    mine = jnp.where(k_core == core, spot, -1)
    theirs = jnp.where(k_core == core, -1, spot)
    from_twin = send(sketches, SWAP)
    twin_spot = send(theirs, SWAP)
    slots = iota((2 * rows_dev, rows_dev), 0)
    table_own = (slots == mine[None, :]).astype(BF16)
    table_twin = (slots == twin_spot[None, :]).astype(BF16)
    outgoing = (
        jnp.dot(table_own, sketches, preferred_element_type=F32)
        + jnp.dot(table_twin, from_twin, preferred_element_type=F32)
    ).astype(BF16)
    own = lax.all_to_all(
        outgoing.reshape(8, 64, width), AX, 0, 0, axis_index_groups=regroup_groups(), tiled=True
    ).reshape(512, width)

    edges = [0]
    for size in CHUNKS:
        edges.append(edges[-1] + width // sum(CHUNKS) * size)
    o, l, r, f = [], [], [], []
    for lo, hi in zip(edges, edges[1:]):
        part = own[:, lo:hi]
        o.append(part)
        l.append(send(part, UP))
        r.append(send(part, DOWN))
        f.append(send(jnp.where(edge == 0, l[-1], part), ACROSS))

    src, member, slot = source_of(None, x, z, y, core, iota((1, 512), 1))
    place = member * 512 + src * 4 + slot
    seen = jnp.sum(
        jnp.where(iota((128, 512), 0) == src, exact(host_counts.T, (iota((8, 512), 0) == member).astype(F32)), 0.0),
        axis=0,
    )
    valid = slot[0].astype(F32) < seen
    n_valid = jnp.sum(host_counts)
    hit = (place == jnp.concatenate([picks, -jnp.ones((5,), jnp.int32)])[:, None]).astype(BF16)
    found = jnp.dot(hit, own, preferred_element_type=F32).astype(BF16)
    found = lax.all_gather(found, AX, axis_index_groups=class_groups())
    found = jnp.sum(found.astype(F32), axis=0).astype(BF16)
    to_picks = inner(found, own)
    pick_half = 0.5 * jnp.sum(jnp.square(found.astype(F32)), axis=1)
    half = 0.5 * jnp.sum(jnp.square(own.astype(F32)), axis=1)
    near = pick_half[:3, None] - to_picks[:3]
    near1 = near[0]
    near2 = jnp.minimum(near[0], near[1])
    near3 = jnp.minimum(near2, near[2])
    info = jnp.stack(
        [half, jnp.where(valid, half, -BIG), jnp.where(valid, near1, -BIG), jnp.where(valid, near2, -BIG)]
    )
    info_l = send(info, UP)
    info_r = send(info, DOWN)
    info_f = send(info, FOURTH)

    def product(a, b):
        total = inner(a[0], b[0])
        for u, v in zip(a[1:], b[1:]):
            total = total + inner(u, v)
        return total

    oo, ol, lr, fr, fo = product(o, o), product(o, l), product(l, r), product(f, r), product(f, o)
    to_o = reach(oo, info, info) + reach(ol.T, info_l, info) + reach(fo, info_f, info)
    to_l = reach(ol, info, info_l)
    to_r = reach(lr, info_l, info_r) + reach(fr, info_f, info_r)
    to_f = reach(fr.T, info_r, info_f) + reach(fo.T, info, info_f)
    bound = jnp.maximum(
        jnp.max(
            jnp.stack(
                [
                    furthest(oo, info, info),
                    furthest(ol, info, info_l),
                    furthest(lr, info_l, info_r),
                    furthest(fr, info_f, info_r),
                    furthest(fo, info_f, info),
                ]
            )
        ),
        0.0,
    )
    to_o = to_o.at[0].add(-n_valid * half)
    extra = jnp.stack(
        [half + near3, jnp.broadcast_to(bound, (512,)), jnp.broadcast_to(jnp.sum(half), (512,)), jnp.zeros((512,), F32)]
    )
    given = jnp.concatenate([jnp.stack([to_o, to_l, to_r, to_f]), extra[:, None, :]], axis=1)

    lane = iota((512, 512), 0)
    to_lane = (lane // 4 % 8) * 64 + (lane // 32) * 4 + lane % 4
    by_member = (to_lane == iota((512, 512), 1)).astype(F32)
    given = exact(given.reshape(16, 512), by_member)
    given = given.reshape(16, 8, 64).transpose(1, 0, 2)
    zl_p, edge_p = iota((4, 1, 1), 0) // 2, iota((4, 1, 1), 0) % 2
    wanted = jnp.where(first, edge_p * 2 + zl_p == z, zl_p * 2 + edge_p == x)
    outbox = jnp.where(wanted[None], given[:, None], 0.0).reshape(32, 16, 64)
    inbox = lax.all_to_all(outbox, AX, 0, 0, axis_index_groups=final_groups(), tiled=True)
    inbox = inbox.reshape(4, 4, 2, 4, 4, 64)
    inbox = jnp.where(first, jnp.sum(inbox, axis=1), jnp.sum(inbox, axis=0))
    o_part, l_part, r_part, f_part = (inbox[:, :, b] for b in range(4))
    total3 = o_part[:, :, :3] + jnp.roll(l_part[:, :, :3], -1, axis=0) + jnp.roll(r_part[:, :, :3], 1, axis=0)
    f_home = jnp.stack([jnp.roll(f_part[:, 1, :3], -1, axis=0), f_part[:, 0, :3]], axis=1)
    total3 = total3 + f_home
    merged = jnp.concatenate([total3, o_part[:, :, 3:4]], axis=2)
    far = 2.0 * jnp.max(l_part[:, :, 3])
    half_sum = jnp.sum(r_part[:, :, 3, 0])
    flat = merged.transpose(2, 0, 1, 3).reshape(4, 512)

    lane1 = iota((512, 1), 0)
    line, sd, rest = lane1 // 128, lane1 // 64 % 2, lane1 % 64
    pair_y0 = y // 2 * 2 + sd
    pair_low = (y == 1) | (y == 2)
    pair_y1 = jnp.where(pair_low, 2 - sd, 3 * sd)
    pair_y = jnp.where(first, pair_y0, pair_y1)
    src2, _, slot2 = source_of(None, line, line, pair_y, core, (rest // 4) * 32 + rest % 4)
    order = (src2 * 4 + slot2 == iota((512, 512), 1)).astype(F32)
    final = exact(flat, order)

    class_counts = counts[0]
    own_counts = lax.dynamic_index_in_dim(class_counts, dp, 0, keepdims=False)
    keep = (iota((128, 4), 1) < own_counts[:, None]).reshape(512).astype(F32)
    total = jnp.sum(class_counts).astype(F32)
    gain0 = (2.0 * final[0] + total * far - 2.0 * half_sum) / width
    gains = jnp.stack([gain0, 2.0 * final[1] / width, 2.0 * final[2] / width])
    gain_scores = (gains * keep[None, :] / total)[:, None, :]
    coverage = (keep * (far - 2.0 * final[3]) / width)[None, :]
    return (gain_scores, coverage)


def solution(mesh):
    placed = (
        P(("dp", "cls"), None),
        P(("dp", "cls")),
        P(("dp", "cls")),
        P("cls", None, None),
        P(None, "cls"),
    )
    return jax.shard_map(
        body,
        mesh=mesh,
        in_specs=placed,
        out_specs=(P(None, "cls", "dp"), P("cls", "dp")),
        check_vma=False,
    )
```

```python
import functools

import jax
import jax.numpy as jnp
from jax import lax
from jax.experimental import pallas as pl
from jax.experimental.pallas import tpu as pltpu
from jax.sharding import PartitionSpec as P


AX = ("dp", "cls")
F32 = jnp.float32
BF16 = jnp.bfloat16
BIG = 1e30
CHUNKS = (128, 128, 256)
STEP = 64
PARTS = 1


def dix(x, y, z, c):
    return x * 32 + (z // 2) * 16 + (z % 2) * 8 + y * 2 + c


def xyz(d):
    return d // 32, (d // 2) % 4, ((d // 16) % 2) * 2 + (d // 8) % 2, d % 2


DEV = range(128)
MATE = ((1, 0, 3, 2), (3, 2, 1, 0))
PAIRS = (((0, 1), (2, 3)), ((2, 1), (0, 3)))


def mate(d):
    x, y, z, c = xyz(d)
    return dix(x, MATE[c][y], z, c)


def along(d, k):
    x, y, z, c = xyz(d)
    return dix((x + k) % 4, y, z, c) if c == 0 else dix(x, y, (z + k) % 4, c)


def side(d):
    return xyz(d)[1] % 2


SWAP = [(d, d ^ 1) for d in DEV]
UP = [(d, along(d, 1)) for d in DEV]
DOWN = [(d, along(d, -1)) for d in DEV]
ACROSS = [(d, mate(d)) for d in DEV]
FOURTH = [(d, mate(d) if side(d) == 1 else mate(along(d, 1))) for d in DEV]


def regroup_groups():
    groups = []
    for x in range(4):
        for ys in ((0, 3), (1, 2)):
            groups.append([dix(x, y, z, 0) for y in ys for z in range(4)])
    for z in range(4):
        for ys in ((1, 0), (2, 3)):
            groups.append([dix(x, y, z, 1) for y in ys for x in range(4)])
    return groups


def class_groups():
    groups = []
    for c in (0, 1):
        for pair in PAIRS[c]:
            for u in range(4):
                group = [dix(t, y, u, 0) if c == 0 else dix(u, y, t, 1) for t in range(4) for y in pair]
                groups.append(group)
    return groups


def final_groups():
    groups = []
    for c in (0, 1):
        for pair in PAIRS[c]:
            groups.append([dix(x, y, z, c) for x in range(4) for z in range(4) for y in pair])
    return groups


def info_pairs():
    out = []
    for d in DEV:
        x, y, z, c = xyz(d)
        zh, zl = z // 2, z % 2
        if c == 0:
            src = dix(x, (y // 2) * 2 + zh, (y % 2) * 2 + zl, 0)
        else:
            yk = y if y % 2 == x % 2 else MATE[1][y]
            src = dix(zh * 2 + zl, yk, (y % 2) * 2 + x // 2, 1)
        out.append((src, d))
    return out


INFO = info_pairs()


def send(value, pairs):
    return lax.ppermute(value, AX, pairs)


def iota(shape, dim):
    return lax.broadcasted_iota(jnp.int32, shape, dim)


def inner(left, right):
    return lax.dot_general(left, right, (((1,), (1,)), ((), ())), preferred_element_type=F32)


def exact(left, right):
    return jnp.dot(left, right, precision=lax.Precision.HIGHEST, preferred_element_type=F32)


def exact_dot(left, right, dims=(((1,), (0,)), ((), ()))):
    return lax.dot_general(left, right, dims, precision=lax.Precision.HIGHEST, preferred_element_type=F32)


def split3(value):
    high = value.astype(BF16)
    rest = value - high.astype(F32)
    middle = rest.astype(BF16)
    return high, middle, (rest - middle.astype(F32)).astype(BF16)


def pair_work(tasks, q_parts, groups, hbm, note_refs, col_refs, q_buf, u_bufs, x_ref, side_ref, sems):
    copies = {}
    count = 0
    width = q_buf.shape[1]
    cuts = [slice(h * width // PARTS, (h + 1) * width // PARTS) for h in range(PARTS)]
    for kind, parts, bufs in (("q", q_parts, [q_buf] * len(q_parts)), ("u", groups, u_bufs)):
        for i, members in enumerate(parts):
            if members is None:
                continue
            at = i * 512 if kind == "q" else 0
            for name in members:
                k = hbm[name].shape[0]
                for h, cut in enumerate(cuts):
                    copy = pltpu.make_async_copy(hbm[name].at[:, cut], bufs[i].at[at : at + k, cut], sems.at[count])
                    copies.setdefault((kind, i, h), []).append(copy)
                    count += 1
                at += k
    begun = []
    for g, rows in tasks:
        for h in range(PARTS):
            for key in [("u", g, h)] + [("q", q, h) for q, _, _ in rows]:
                if key in copies and key not in begun:
                    begun.append(key)
                    for copy in copies[key]:
                        copy.start()
    for q in range(len(q_parts)):
        parts = jnp.concatenate([p.astype(F32) for p in split3(note_refs[q][...])], axis=0).astype(BF16)
        along = (iota((24, 512), 0) % 8 == iota((24, 512), 1) // 128).astype(BF16)
        wide = lax.dot_general(parts, along, (((0,), (0,)), ((), ())), preferred_element_type=F32)
        for j in range(4):
            side_ref[q, j] = wide[:, j * 128 : j * 128 + 128]
    ready = set()
    fresh = set(col_refs)
    far = jnp.zeros((8, 128), F32)
    lanes = {}
    for g, given in tasks:
        data = q_buf if groups[g] is None else u_bufs[g]
        m = 512 if groups[g] is None else data.shape[0]
        lo, hi = 512 * given[0][0], 512 * given[-1][0] + 512
        tiles = m // 128
        u_half, u_mark, u_one, u_two = [
            [
                jnp.broadcast_to(note_refs[len(q_parts) + g][i : i + 1, t * 128 : t * 128 + 128], (8, 128))
                for t in range(tiles)
            ]
            for i in range(4)
        ]
        for h, cut in enumerate(cuts):
            for key in [("u", g, h)] + [("q", q, h) for q, _, _ in given]:
                if key in copies and key not in ready:
                    ready.add(key)
                    for copy in copies[key]:
                        copy.wait()
            part = lax.dot_general(
                q_buf[lo:hi, cut], data[:m, cut], (((1,), (1,)), ((), ())), preferred_element_type=F32
            )
            if h == 0:
                x_ref[lo:hi, :m] = part
            else:
                x_ref[lo:hi, :m] += part
        for q, to_u, to_q in given:
            first_use = to_q and q in fresh
            if to_q:
                fresh.discard(q)

            def step(i, carry, q=q, to_u=to_u, to_q=to_q, first_use=first_use, tiles=tiles, u=(u_half, u_mark, u_one, u_two)):
                carry = [list(c) for c in carry]
                u_half, u_mark, u_one, u_two = u
                start = pl.multiple_of(i * STEP, STEP)
                for k in range(STEP // 8):
                    rows = pl.ds(start + k * 8, 8)
                    q_half, q_mark, q_one, q_two = (side_ref[q, j, rows, :] for j in range(4))
                    sums = [None, None, None]
                    for t in range(tiles):
                        x = x_ref[pl.ds(start + (q * 512 + k * 8), 8), t * 128 : t * 128 + 128]
                        carry[0][t] = jnp.maximum(carry[0][t], (q_mark - x) + u_mark[t])
                        if to_u:
                            carry[1][t] = carry[1][t] + x
                            carry[2][t] = carry[2][t] + jnp.maximum((x + q_one) - u_half[t], 0.0)
                            carry[3][t] = carry[3][t] + jnp.maximum((x + q_two) - u_half[t], 0.0)
                        if to_q:
                            off = x - q_half
                            values = (x, jnp.maximum(off + u_one[t], 0.0), jnp.maximum(off + u_two[t], 0.0))
                            sums = [v if s is None else s + v for s, v in zip(sums, values)]
                    if to_q:
                        for j in range(3):
                            if first_use:
                                col_refs[q][j, rows, :] = sums[j]
                            else:
                                col_refs[q][j, rows, :] += sums[j]
                return carry

            zero = [jnp.zeros((8, 128), F32)] * tiles
            done = lax.fori_loop(0, 512 // STEP, step, [zero] * (4 if to_u else 1))
            for t in range(tiles):
                far = jnp.maximum(far, done[0][t])
            if to_u:
                done = done[1:]
                lanes[g] = [[a + b for a, b in zip(v, w)] for v, w in zip(lanes[g], done)] if g in lanes else done
    rows = {
        g: [
            jnp.concatenate([jnp.sum(v, axis=0, keepdims=True) for v in kind], axis=1) for kind in value
        ]
        for g, value in lanes.items()
    }
    return rows, far


def scratch_for(q_parts, groups, sizes, width):
    q_bufs = [pltpu.VMEM((512 * len(q_parts), width), BF16)]
    u_sizes = [sum(sizes[i] for i in p) if p else 0 for p in groups]
    u_bufs = [pltpu.VMEM((n or 16, width), BF16) for n in u_sizes]
    n_copies = sum(len(p) for p in q_parts) + sum(len(p) for p in groups if p)
    most = max([n or 512 for n in u_sizes])
    return q_bufs + u_bufs + [
        pltpu.VMEM((512 * len(q_parts), most), F32),
        pltpu.VMEM((len(q_parts), 4, 512, 128), F32),
        pltpu.SemaphoreType.DMA((n_copies * PARTS,)),
    ]


def cost_of(tasks, q_parts, groups, sizes, width):
    def rows(p):
        return sum(sizes[i] for i in (p or q_parts[0]))

    flops = sum(2 * 512 * len(t[1]) * rows(groups[t[0]]) * width for t in tasks)
    moved = 2 * width * sum(sizes)
    return pl.CostEstimate(flops=flops, transcendentals=0, bytes_accessed=moved)


VMEM_SPEC = pl.BlockSpec(memory_space=pltpu.VMEM)
ANY_SPEC = pl.BlockSpec(memory_space=pl.ANY)
LIMIT = pltpu.CompilerParams(vmem_limit_bytes=36 * 2**20)


def early_kernel(tasks, q_parts, groups, n_hbm, lane_outs, col_outs, *refs):
    hbm, refs = refs[:n_hbm], refs[n_hbm:]
    n_notes = len(q_parts) + len(groups)
    notes, refs = refs[:n_notes], refs[n_notes:]
    lane_refs, refs = refs[: len(lane_outs)], refs[len(lane_outs) :]
    cols, refs = dict(zip(col_outs, refs)), refs[len(col_outs) :]
    far_ref, refs = refs[0], refs[1:]
    q_buf, refs = refs[0], refs[1:]
    u_bufs, (x_ref, side_ref, sems) = refs[: len(groups)], refs[len(groups) :]
    rows, far = pair_work(tasks, q_parts, groups, hbm, notes, cols, q_buf, u_bufs, x_ref, side_ref, sems)
    for g, ref in zip(lane_outs, lane_refs):
        ref[...] = jnp.zeros_like(ref)
        for j in range(3):
            ref[j : j + 1, :] = rows[g][j]
    far_ref[...] = far


def early_pairs(hbm, q_parts, groups, notes, tasks):
    sizes, width = [h.shape[0] for h in hbm], hbm[0].shape[1]
    lane_outs = [t[0] for t in tasks if any(v[1] for v in t[1])]
    col_outs = [q for q in range(len(q_parts)) if any(v[0] == q and v[2] for t in tasks for v in t[1])]
    shapes = [jax.ShapeDtypeStruct((8, notes[len(q_parts) + g].shape[1]), F32) for g in lane_outs]
    shapes += [jax.ShapeDtypeStruct((3, 512, 128), F32) for _ in col_outs]
    shapes += [jax.ShapeDtypeStruct((8, 128), F32)]
    out = pl.pallas_call(
        functools.partial(early_kernel, tasks, q_parts, groups, len(hbm), lane_outs, col_outs),
        out_shape=shapes,
        in_specs=[ANY_SPEC] * len(hbm) + [VMEM_SPEC] * len(notes),
        out_specs=[VMEM_SPEC] * len(shapes),
        scratch_shapes=scratch_for(q_parts, groups, sizes, width),
        cost_estimate=cost_of(tasks, q_parts, groups, sizes, width),
        compiler_params=LIMIT,
    )(*hbm, *notes)
    n = len(lane_outs)
    return dict(zip(lane_outs, out)), dict(zip(col_outs, out[n:])), out[-1]


def last_kernel(tasks, q_parts, groups, n_hbm, lane_rows, n_cols, n_far, own_rows, *refs):
    hbm, refs = refs[:n_hbm], refs[n_hbm:]
    n_notes = len(q_parts) + len(groups)
    notes, refs = refs[:n_notes], refs[n_notes:]
    lane_refs, refs = refs[: len(lane_rows)], refs[len(lane_rows) :]
    col_refs, refs = refs[: sum(n_cols)], refs[sum(n_cols) :]
    far_refs, refs = refs[:n_far], refs[n_far:]
    extra_ref, out_ref, refs = refs[0], refs[1], refs[2:]
    q_buf, refs = refs[0], refs[1:]
    u_bufs, refs = refs[: len(groups)], refs[len(groups) :]
    x_ref, side_ref, sems, col0_ref, col1_ref, g_ref = refs
    cols = {0: col0_ref, 1: col1_ref}
    rows, far = pair_work(tasks, q_parts, groups, hbm, notes, cols, q_buf, u_bufs, x_ref, side_ref, sems)
    g_ref[...] = extra_ref[...]
    for ref, (row, at) in zip(lane_refs, lane_rows):
        m = ref.shape[1]
        g_ref[row : row + 3, at : at + m] += ref[0:3, :]
    for g, (row, at) in own_rows.items():
        for j in range(3):
            value = rows[g][j]
            g_ref[row + j : row + j + 1, at : at + value.shape[1]] += value
    start = 0
    for q, (n, row) in enumerate(zip(n_cols, (0, 8))):
        for j in range(3):
            total = cols[q][j]
            for ref in col_refs[start : start + n]:
                total = total + ref[j]
            across = jnp.sum(jnp.transpose(total), axis=0, keepdims=True)
            g_ref[row + j : row + j + 1, :] += across
        start += n
    for ref in far_refs:
        far = jnp.maximum(far, ref[...])
    far = jnp.max(jnp.max(far, axis=0, keepdims=True), axis=1, keepdims=True)
    g_ref[7:8, :] = jnp.broadcast_to(far, (1, 512))
    lane = iota((512, 512), 0)
    to_lane = (lane // 4 % 8) * 64 + (lane // 32) * 4 + lane % 4
    by_member = (to_lane == iota((512, 512), 1)).astype(BF16)
    parts = jnp.concatenate([p.astype(F32) for p in split3(g_ref[...])], axis=0).astype(BF16)
    given = jnp.dot(parts, by_member, preferred_element_type=F32)
    given = given[0:16] + given[16:32] + given[32:48]
    for m in range(8):
        piece = given[:, m * 64 : m * 64 + 64]
        page = jnp.concatenate([piece[0:8], piece[8:16]], axis=1)
        for copy in range(4):
            out_ref[m * 4 + copy] = page


def last_pairs(hbm, q_parts, groups, notes, tasks, lanes, lane_rows, cols, fars, own_rows, extra):
    sizes, width = [h.shape[0] for h in hbm], hbm[0].shape[1]
    n_cols = tuple(len(c) for c in cols)
    small = lanes + [c for each in cols for c in each] + fars + [extra]
    return pl.pallas_call(
        functools.partial(
            last_kernel, tasks, q_parts, groups, len(hbm), lane_rows, n_cols, len(fars), own_rows
        ),
        out_shape=jax.ShapeDtypeStruct((32, 8, 128), F32),
        in_specs=[ANY_SPEC] * len(hbm) + [VMEM_SPEC] * (len(notes) + len(small)),
        out_specs=VMEM_SPEC,
        scratch_shapes=scratch_for(q_parts, groups, sizes, width)
        + [pltpu.VMEM((3, 512, 128), F32), pltpu.VMEM((3, 512, 128), F32), pltpu.VMEM((16, 512), F32)],
        cost_estimate=cost_of(tasks, q_parts, groups, sizes, width),
        compiler_params=LIMIT,
    )(*hbm, *notes, *small)


def prep_kernel(own_ref, hit_ref, found_ref, half_ref, buf, part, sems):
    slab = 128
    n = buf.shape[0] // slab
    copies = [
        pltpu.make_async_copy(own_ref.at[i * slab : i * slab + slab, :], buf.at[i * slab : i * slab + slab, :], sems.at[i])
        for i in range(n)
    ]
    for copy in copies:
        copy.start()
    for i, copy in enumerate(copies):
        copy.wait()

        def step(k, _, i=i):
            rows = pl.ds(pl.multiple_of(i * slab + k * 16, 16), 16)
            total = None
            for t in range(buf.shape[1] // 128):
                v = buf[rows, t * 128 : t * 128 + 128].astype(F32)
                total = v * v if total is None else total + v * v
            part[rows, :] = total
            return 0

        lax.fori_loop(0, slab // 16, step, 0)
    half_ref[...] = 0.5 * jnp.sum(jnp.transpose(part[...]), axis=0, keepdims=True)
    found = jnp.dot(hit_ref[...], buf[...], preferred_element_type=F32).astype(BF16)
    for i in range(8):
        found_ref[i] = found


def prepare(own, hit):
    width = own.shape[1]
    return pl.pallas_call(
        prep_kernel,
        out_shape=[jax.ShapeDtypeStruct((8, 8, width), BF16), jax.ShapeDtypeStruct((1, 512), F32)],
        in_specs=[ANY_SPEC, VMEM_SPEC],
        out_specs=[VMEM_SPEC, VMEM_SPEC],
        scratch_shapes=[pltpu.VMEM((512, width), BF16), pltpu.VMEM((512, 128), F32), pltpu.SemaphoreType.DMA((4,))],
        cost_estimate=pl.CostEstimate(flops=2 * 512 * 512 * width, transcendentals=0, bytes_accessed=own.size * 2),
        compiler_params=LIMIT,
    )(own, hit)


def close_kernel(width, where_ref, in_ref, order_ref, keep_ref, total_ref, gain_ref, cover_ref):
    lane = iota((4, 128), 1)
    row = iota((4, 128), 0)

    def page(line, sd):
        return in_ref[where_ref[0] + where_ref[1] * (line % 4) + sd]

    final = jnp.zeros((8, 512), F32)
    far = jnp.zeros((1, 64), F32)
    half_sum = jnp.zeros((1, 64), F32)
    for line in range(4):
        for sd in range(2):
            here = page(line, sd)
            far = jnp.maximum(far, here[7:8, 0:64])
            half_sum = half_sum + here[3:4, 64:128]
            low = here[0:4] + jnp.where(row < 3, page(line + 1, sd)[4:8], 0.0)
            fourth = page(line, 0) if sd == 1 else page(line + 1, 1)
            high = jnp.where(row < 3, page(line + 3, sd)[0:4] + fourth[4:8], 0.0)
            both = jnp.where(lane < 64, low, high)
            both = both[:, 0:64] + both[:, 64:128]
            both = jnp.concatenate([both, jnp.zeros((4, 64), F32)], axis=0)
            at = (line * 2 + sd) * 64
            final = final + exact_dot(both, order_ref[at : at + 64, :])
    far = 2.0 * far[:, 0:1]
    half_sum = half_sum[:, 0:1]
    keep = keep_ref[...]
    total = total_ref[:, 0:1]
    scale = 1.0 / width
    gain_ref[0:1, :] = (2.0 * final[0:1] + total * far - 2.0 * half_sum) * scale * keep / total
    gain_ref[1:3, :] = 2.0 * final[1:3] * scale * keep / total
    cover_ref[...] = keep * (far - 2.0 * final[3:4]) * scale


def source_of(x, z, y, core, row):
    group, sub, member, slot = row // 64, row // 32 % 2, row // 4 % 8, row % 4
    i, w = group // 4, group % 4
    outer = (y == 0) | (y == 3)
    low = y < 2
    y0 = jnp.where(outer, 3 * i, 1 + i)
    y1 = jnp.where(low, 1 - i, 2 + i)
    sx = jnp.where(core == 0, x, w)
    sz = jnp.where(core == 0, w, z)
    sy = jnp.where(core == 0, y0, y1)
    return dix(sx, sy, sz, jnp.where(sub == 0, 0, 1)), member, slot


def body(sketches, labels, places, counts, chosen):
    rows_dev, width = sketches.shape
    dp, cls = lax.axis_index("dp"), lax.axis_index("cls")
    x, zh, zl, y, core = dp // 2, dp % 2, cls // 8, cls // 2 % 4, cls % 2
    z = zh * 2 + zl
    edge = y % 2
    first = core == 0

    packed = jnp.concatenate([counts[0], jnp.broadcast_to(chosen, (3, 128))], axis=0)
    packed = send(packed, INFO)
    host_counts = packed[:8].astype(F32)
    picks = packed[8:11, 0]

    k_core, k_y, k_zl = labels % 2, labels // 2 % 4, labels // 8
    group = jnp.where(
        k_core == 0,
        (k_y // 2) * 4 + (k_y % 2) * 2 + k_zl,
        ((k_y + 3) % 4 // 2) * 4 + k_zl * 2 + k_y % 2,
    )
    spot = group * 64 + core * 32 + places // 512 * 4 + places % 4
    mine = jnp.where(k_core == core, spot, -1)
    theirs = jnp.where(k_core == core, -1, spot)
    from_twin = send(sketches, SWAP)
    twin_spot = send(theirs, SWAP)
    slots = iota((2 * rows_dev, rows_dev), 0)
    table_own = (slots == mine[None, :]).astype(BF16)
    table_twin = (slots == twin_spot[None, :]).astype(BF16)
    outgoing = (
        jnp.dot(table_own, sketches, preferred_element_type=F32)
        + jnp.dot(table_twin, from_twin, preferred_element_type=F32)
    ).astype(BF16)
    own = lax.all_to_all(
        outgoing.reshape(8, 64, width), AX, 0, 0, axis_index_groups=regroup_groups(), tiled=True
    ).reshape(512, width)

    src, member, slot = source_of(x, z, y, core, iota((1, 512), 1))
    place = member * 512 + src * 4 + slot
    seen = jnp.sum(
        jnp.where(iota((128, 512), 0) == src, exact(host_counts.T, (iota((8, 512), 0) == member).astype(F32)), 0.0),
        axis=0,
    )
    valid = slot[0].astype(F32) < seen
    n_valid = jnp.sum(host_counts)
    hit = (place == jnp.concatenate([picks, -jnp.ones((5,), jnp.int32)])[:, None]).astype(BF16)
    found, half = prepare(own, hit)
    half = half[0]
    edges = [0]
    for size in CHUNKS:
        edges.append(edges[-1] + size)
    spans = list(zip(edges, edges[1:]))
    l, f = [], []
    late, found = lax.optimization_barrier((own, found))
    cuts = [(late if lo else own)[lo:hi] for lo, hi in spans]
    for cut in cuts:
        l.append(send(cut, UP))
    for i, cut in enumerate(cuts):
        f.append(send(jnp.where(edge == 0, l[i], cut), ACROSS))
    r = []
    for cut in cuts:
        r.append(send(cut, DOWN))

    found = lax.all_to_all(found, AX, 0, 0, axis_index_groups=class_groups(), tiled=True)
    found = jnp.sum(found.astype(F32), axis=0).astype(BF16)
    to_picks = inner(found, own)
    pick_half = 0.5 * jnp.sum(jnp.square(found.astype(F32)), axis=1)
    near = pick_half[:3, None] - to_picks[:3]
    near1 = near[0]
    near2 = jnp.minimum(near[0], near[1])
    near3 = jnp.minimum(near2, near[2])
    info = jnp.stack(
        [half, jnp.where(valid, half, -BIG), jnp.where(valid, near1, -BIG), jnp.where(valid, near2, -BIG)]
        + [jnp.zeros((512,), F32)] * 4
    )
    info_l = send(info, UP)
    info_r = send(info, DOWN)
    info_f = send(info, FOURTH)

    mid = edges[2]
    l_low, l_high = info_l[:, :mid], info_l[:, mid:]
    f_low, f_high = info_f[:, :mid], info_f[:, mid:]
    lanes_a, cols_a, far_a = early_pairs(
        [own, l[0], l[1]],
        [[0]],
        [None, [1, 2]],
        [info, info, l_low],
        [(0, [(0, True, False)]), (1, [(0, True, True)])],
    )
    lanes_b, cols_b, far_b = early_pairs(
        [own, *r, *l, f[0], f[1]],
        [[0], [1, 2, 3]],
        [[7, 8], [6], [4, 5]],
        [info, info_r, f_low, l_high, l_low],
        [(0, [(0, True, True), (1, True, True)]), (1, [(0, True, True), (1, False, True)]), (2, [(1, False, True)])],
    )
    none = jnp.zeros((512,), F32)
    extra = [none] * 16
    extra[0] = -n_valid * half
    extra[3] = half + near3
    extra[11] = jnp.broadcast_to(jnp.sum(half), (512,))
    extra = jnp.stack(extra)
    lane_list = [
        (lanes_a[0], (0, 0)),
        (lanes_a[1], (4, 0)),
        (lanes_b[0], (12, 0)),
        (lanes_b[1], (4, mid)),
    ]
    outbox = last_pairs(
        [own, *r, f[2]],
        [[0], [1, 2, 3]],
        [[4]],
        [info, info_r, f_high],
        [(0, [(0, True, True), (1, True, True)])],
        [v for v, _ in lane_list],
        [at for _, at in lane_list],
        [[cols_a[0], cols_b[0]], [cols_b[1]]],
        [far_a, far_b],
        {0: (12, mid)},
        extra,
    )
    inbox = lax.all_to_all(outbox, AX, 0, 0, axis_index_groups=final_groups(), tiled=True)

    lane1 = iota((512, 1), 0)
    line, sd, rest = lane1 // 128, lane1 // 64 % 2, lane1 % 64
    pair_y0 = y // 2 * 2 + sd
    pair_low = (y == 1) | (y == 2)
    pair_y1 = jnp.where(pair_low, 2 - sd, 3 * sd)
    pair_y = jnp.where(first, pair_y0, pair_y1)
    src2, _, slot2 = source_of(line, line, pair_y, core, (rest // 4) * 32 + rest % 4)
    in_order = (src2 * 4 + slot2 == iota((512, 512), 1)).astype(F32)

    class_counts = counts[0]
    own_counts = lax.dynamic_index_in_dim(class_counts, dp, 0, keepdims=False)
    keep = (iota((128, 4), 1) < own_counts[:, None]).reshape(1, 512).astype(F32)
    total = jnp.broadcast_to(jnp.sum(class_counts).astype(F32), (1, 128))
    host = jnp.where(first, (edge * 2 + zl) * 2, (zl * 2 + edge) * 8)
    where = jnp.stack([host, jnp.where(first, 8, 2)])
    gains, cover = pl.pallas_call(
        functools.partial(close_kernel, width),
        out_shape=[jax.ShapeDtypeStruct((3, 512), F32), jax.ShapeDtypeStruct((1, 512), F32)],
        in_specs=[pl.BlockSpec(memory_space=pltpu.SMEM)] + [VMEM_SPEC] * 4,
        out_specs=[VMEM_SPEC, VMEM_SPEC],
    )(where, inbox, in_order, keep, total)
    return (gains[:, None, :], cover)


def solution(mesh):
    placed = (
        P(("dp", "cls"), None),
        P(("dp", "cls")),
        P(("dp", "cls")),
        P("cls", None, None),
        P(None, "cls"),
    )
    return jax.shard_map(
        body,
        mesh=mesh,
        in_specs=placed,
        out_specs=(P(None, "cls", "dp"), P("cls", "dp")),
        check_vma=False,
    )
```

```python
import functools

import jax
import jax.numpy as jnp
from jax import lax
from jax.experimental import pallas as pl
from jax.experimental.pallas import tpu as pltpu
from jax.sharding import PartitionSpec as P


AX = ("dp", "cls")
F32 = jnp.float32
BF16 = jnp.bfloat16
BIG = 1e30
STEP = 64


def dix(x, y, z, c):
    return x * 32 + (z // 2) * 16 + (z % 2) * 8 + y * 2 + c


def xyz(d):
    return d // 32, (d // 2) % 4, ((d // 16) % 2) * 2 + (d // 8) % 2, d % 2


DEV = range(128)
MATE = ((1, 0, 3, 2), (3, 2, 1, 0))
PAIRS = (((0, 1), (2, 3)), ((2, 1), (0, 3)))


def mate(d):
    x, y, z, c = xyz(d)
    return dix(x, MATE[c][y], z, c)


def along(d, k):
    x, y, z, c = xyz(d)
    return dix((x + k) % 4, y, z, c) if c == 0 else dix(x, y, (z + k) % 4, c)


def side(d):
    return xyz(d)[1] % 2


SWAP = [(d, d ^ 1) for d in DEV]
UP = [(d, along(d, 1)) for d in DEV]
DOWN = [(d, along(d, -1)) for d in DEV]
ACROSS = [(d, mate(d)) for d in DEV]
FOURTH = [(d, mate(d) if side(d) == 1 else mate(along(d, 1))) for d in DEV]


def regroup_groups():
    groups = []
    for x in range(4):
        for ys in ((0, 3), (1, 2)):
            groups.append([dix(x, y, z, 0) for y in ys for z in range(4)])
    for z in range(4):
        for ys in ((1, 0), (2, 3)):
            groups.append([dix(x, y, z, 1) for y in ys for x in range(4)])
    return groups


def class_groups():
    groups = []
    for c in (0, 1):
        for pair in PAIRS[c]:
            for u in range(4):
                group = [dix(t, y, u, 0) if c == 0 else dix(u, y, t, 1) for t in range(4) for y in pair]
                groups.append(group)
    return groups


def final_groups():
    groups = []
    for c in (0, 1):
        for pair in PAIRS[c]:
            groups.append([dix(x, y, z, c) for x in range(4) for z in range(4) for y in pair])
    return groups


def info_pairs():
    out = []
    for d in DEV:
        x, y, z, c = xyz(d)
        zh, zl = z // 2, z % 2
        if c == 0:
            src = dix(x, (y // 2) * 2 + zh, (y % 2) * 2 + zl, 0)
        else:
            yk = y if y % 2 == x % 2 else MATE[1][y]
            src = dix(zh * 2 + zl, yk, (y % 2) * 2 + x // 2, 1)
        out.append((src, d))
    return out


INFO = info_pairs()


def send(value, pairs):
    return lax.ppermute(value, AX, pairs)


def iota(shape, dim):
    return lax.broadcasted_iota(jnp.int32, shape, dim)


def inner(left, right):
    return lax.dot_general(left, right, (((1,), (1,)), ((), ())), preferred_element_type=F32)


def exact(left, right):
    return jnp.dot(left, right, precision=lax.Precision.HIGHEST, preferred_element_type=F32)


def exact_dot(left, right, dims=(((1,), (0,)), ((), ()))):
    return lax.dot_general(left, right, dims, precision=lax.Precision.HIGHEST, preferred_element_type=F32)


def split3(value):
    high = value.astype(BF16)
    rest = value - high.astype(F32)
    middle = rest.astype(BF16)
    return high, middle, (rest - middle.astype(F32)).astype(BF16)


def pair_work(side, tasks, q_parts, groups, hbm, note_refs, col_refs, q_buf, u_bufs, x_ref, side_ref, sems):
    copies = {}
    count = 0
    for kind, parts, bufs in (("q", q_parts, [q_buf] * len(q_parts)), ("u", groups, u_bufs)):
        for i, members in enumerate(parts):
            if members is None:
                continue
            at = i * 512 if kind == "q" else 0
            for member in members:
                either = isinstance(member, tuple)
                k = hbm[member[2] if either else member].shape[0]
                target = bufs[i].at[at : at + k, :]
                if either:
                    one = pltpu.make_async_copy(hbm[member[0]].at[member[1] : member[1] + k, :], target, sems.at[count])
                    two = pltpu.make_async_copy(hbm[member[2]], target, sems.at[count])
                    copies.setdefault((kind, i), []).append((one, two))
                else:
                    copies.setdefault((kind, i), []).append((pltpu.make_async_copy(hbm[member], target, sems.at[count]),))
                count += 1
                at += k
    begun = []
    for g, rows in tasks:
        for key in [("u", g)] + [("q", q) for q, _, _ in rows]:
            if key in copies and key not in begun:
                begun.append(key)
                for copy in copies[key]:
                    if len(copy) == 1:
                        copy[0].start()
                    else:
                        for choice in (0, 1):
                            pl.when(side == choice)(copy[choice].start)
    for q in range(len(q_parts)):
        parts = jnp.concatenate([p.astype(F32) for p in split3(note_refs[q][...])], axis=0).astype(BF16)
        along = (iota((24, 512), 0) % 8 == iota((24, 512), 1) // 128).astype(BF16)
        wide = lax.dot_general(parts, along, (((0,), (0,)), ((), ())), preferred_element_type=F32)
        for j in range(4):
            side_ref[q, j] = wide[:, j * 128 : j * 128 + 128]
    ready = set()
    fresh = set(col_refs)
    far = jnp.zeros((8, 128), F32)
    lanes = {}
    for g, given in tasks:
        data = q_buf if groups[g] is None else u_bufs[g]
        m = 512 if groups[g] is None else data.shape[0]
        lo, hi = 512 * given[0][0], 512 * given[-1][0] + 512
        tiles = m // 128
        u_half, u_mark, u_one, u_two = [
            [
                jnp.broadcast_to(note_refs[len(q_parts) + g][i : i + 1, t * 128 : t * 128 + 128], (8, 128))
                for t in range(tiles)
            ]
            for i in range(4)
        ]
        for key in [("u", g)] + [("q", q) for q, _, _ in given]:
            if key in copies and key not in ready:
                ready.add(key)
                for copy in copies[key]:
                    copy[0].wait()
        x_ref[lo:hi, :m] = lax.dot_general(
            q_buf[lo:hi], data[:m], (((1,), (1,)), ((), ())), preferred_element_type=F32
        )
        for q, to_u, to_q in given:
            first_use = to_q and q in fresh
            if to_q:
                fresh.discard(q)

            def step(i, carry, q=q, to_u=to_u, to_q=to_q, first_use=first_use, tiles=tiles, u=(u_half, u_mark, u_one, u_two)):
                carry = [list(c) for c in carry]
                u_half, u_mark, u_one, u_two = u
                start = pl.multiple_of(i * STEP, STEP)
                for k in range(STEP // 8):
                    rows = pl.ds(start + k * 8, 8)
                    q_half, q_mark, q_one, q_two = (side_ref[q, j, rows, :] for j in range(4))
                    sums = [None, None, None]
                    for t in range(tiles):
                        x = x_ref[pl.ds(start + (q * 512 + k * 8), 8), t * 128 : t * 128 + 128]
                        carry[0][t] = jnp.maximum(carry[0][t], (q_mark - x) + u_mark[t])
                        if to_u:
                            carry[1][t] = carry[1][t] + x
                            carry[2][t] = carry[2][t] + jnp.maximum((x + q_one) - u_half[t], 0.0)
                            carry[3][t] = carry[3][t] + jnp.maximum((x + q_two) - u_half[t], 0.0)
                        if to_q:
                            off = x - q_half
                            values = (x, jnp.maximum(off + u_one[t], 0.0), jnp.maximum(off + u_two[t], 0.0))
                            sums = [v if s is None else s + v for s, v in zip(sums, values)]
                    if to_q:
                        for j in range(3):
                            if first_use:
                                col_refs[q][j, rows, :] = sums[j]
                            else:
                                col_refs[q][j, rows, :] += sums[j]
                return carry

            zero = [jnp.zeros((8, 128), F32)] * tiles
            done = lax.fori_loop(0, 512 // STEP, step, [zero] * (4 if to_u else 1))
            for t in range(tiles):
                far = jnp.maximum(far, done[0][t])
            if to_u:
                done = done[1:]
                lanes[g] = [[a + b for a, b in zip(v, w)] for v, w in zip(lanes[g], done)] if g in lanes else done
    rows = {
        g: [
            jnp.concatenate([jnp.sum(v, axis=0, keepdims=True) for v in kind], axis=1) for kind in value
        ]
        for g, value in lanes.items()
    }
    return rows, far


def rows_of(part, sizes):
    return sum(sizes[i[2] if isinstance(i, tuple) else i] for i in part)


def scratch_for(q_parts, groups, sizes, width):
    q_bufs = [pltpu.VMEM((512 * len(q_parts), width), BF16)]
    u_sizes = [rows_of(p, sizes) if p else 0 for p in groups]
    u_bufs = [pltpu.VMEM((n or 16, width), BF16) for n in u_sizes]
    n_copies = sum(len(p) for p in q_parts) + sum(len(p) for p in groups if p)
    most = max([n or 512 for n in u_sizes])
    return q_bufs + u_bufs + [
        pltpu.VMEM((512 * len(q_parts), most), F32),
        pltpu.VMEM((len(q_parts), 4, 512, 128), F32),
        pltpu.SemaphoreType.DMA((n_copies,)),
    ]


def cost_of(tasks, q_parts, groups, sizes, width):
    def rows(p):
        return rows_of(p or q_parts[0], sizes)

    flops = sum(2 * 512 * len(t[1]) * rows(groups[t[0]]) * width for t in tasks)
    moved = 2 * width * sum(sizes)
    return pl.CostEstimate(flops=flops, transcendentals=0, bytes_accessed=moved)


VMEM_SPEC = pl.BlockSpec(memory_space=pltpu.VMEM)
SMEM_SPEC = pl.BlockSpec(memory_space=pltpu.SMEM)
ANY_SPEC = pl.BlockSpec(memory_space=pltpu.HBM)
LIMIT = pltpu.CompilerParams(vmem_limit_bytes=36 * 2**20)


def early_kernel(tasks, q_parts, groups, n_hbm, lane_outs, col_outs, side_ref_in, *refs):
    hbm, refs = refs[:n_hbm], refs[n_hbm:]
    n_notes = len(q_parts) + len(groups)
    notes, refs = refs[:n_notes], refs[n_notes:]
    lane_refs, refs = refs[: len(lane_outs)], refs[len(lane_outs) :]
    cols, refs = dict(zip(col_outs, refs)), refs[len(col_outs) :]
    far_ref, refs = refs[0], refs[1:]
    q_buf, refs = refs[0], refs[1:]
    u_bufs, (x_ref, side_ref, sems) = refs[: len(groups)], refs[len(groups) :]
    rows, far = pair_work(side_ref_in[0], tasks, q_parts, groups, hbm, notes, cols, q_buf, u_bufs, x_ref, side_ref, sems)
    for g, ref in zip(lane_outs, lane_refs):
        ref[...] = jnp.zeros_like(ref)
        for j in range(3):
            ref[j : j + 1, :] = rows[g][j]
    far_ref[...] = far


def early_pairs(edge, hbm, q_parts, groups, notes, tasks):
    sizes, width = [h.shape[0] for h in hbm], hbm[0].shape[1]
    lane_outs = [t[0] for t in tasks if any(v[1] for v in t[1])]
    col_outs = [q for q in range(len(q_parts)) if any(v[0] == q and v[2] for t in tasks for v in t[1])]
    shapes = [jax.ShapeDtypeStruct((8, notes[len(q_parts) + g].shape[1]), F32) for g in lane_outs]
    shapes += [jax.ShapeDtypeStruct((3, 512, 128), F32) for _ in col_outs]
    shapes += [jax.ShapeDtypeStruct((8, 128), F32)]
    out = pl.pallas_call(
        functools.partial(early_kernel, tasks, q_parts, groups, len(hbm), lane_outs, col_outs),
        out_shape=shapes,
        in_specs=[SMEM_SPEC] + [ANY_SPEC] * len(hbm) + [VMEM_SPEC] * len(notes),
        out_specs=[VMEM_SPEC] * len(shapes),
        scratch_shapes=scratch_for(q_parts, groups, sizes, width),
        cost_estimate=cost_of(tasks, q_parts, groups, sizes, width),
        compiler_params=LIMIT,
    )(edge.reshape(1), *hbm, *notes)
    n = len(lane_outs)
    return dict(zip(lane_outs, out)), dict(zip(col_outs, out[n:])), out[-1]


def last_kernel(tasks, q_parts, groups, n_hbm, lane_rows, n_cols, n_far, own_rows, side_ref_in, *refs):
    hbm, refs = refs[:n_hbm], refs[n_hbm:]
    n_notes = len(q_parts) + len(groups)
    notes, refs = refs[:n_notes], refs[n_notes:]
    lane_refs, refs = refs[: len(lane_rows)], refs[len(lane_rows) :]
    col_refs, refs = refs[: sum(n_cols)], refs[sum(n_cols) :]
    far_refs, refs = refs[:n_far], refs[n_far:]
    extra_ref, out_ref, refs = refs[0], refs[1], refs[2:]
    q_buf, refs = refs[0], refs[1:]
    u_bufs, refs = refs[: len(groups)], refs[len(groups) :]
    x_ref, side_ref, sems, col0_ref, col1_ref, g_ref = refs
    cols = {0: col0_ref, 1: col1_ref}
    rows, far = pair_work(side_ref_in[0], tasks, q_parts, groups, hbm, notes, cols, q_buf, u_bufs, x_ref, side_ref, sems)
    g_ref[...] = extra_ref[...]
    for ref, (row, at) in zip(lane_refs, lane_rows):
        m = ref.shape[1]
        g_ref[row : row + 3, at : at + m] += ref[0:3, :]
    for g, (row, at) in own_rows.items():
        for j in range(3):
            value = rows[g][j]
            g_ref[row + j : row + j + 1, at : at + value.shape[1]] += value
    start = 0
    for q, (n, row) in enumerate(zip(n_cols, (0, 8))):
        for j in range(3):
            total = cols[q][j]
            for ref in col_refs[start : start + n]:
                total = total + ref[j]
            across = jnp.sum(jnp.transpose(total), axis=0, keepdims=True)
            g_ref[row + j : row + j + 1, :] += across
        start += n
    for ref in far_refs:
        far = jnp.maximum(far, ref[...])
    far = jnp.max(jnp.max(far, axis=0, keepdims=True), axis=1, keepdims=True)
    g_ref[7:8, :] = jnp.broadcast_to(far, (1, 512))
    lane = iota((512, 512), 0)
    to_lane = (lane // 4 % 8) * 64 + (lane // 32) * 4 + lane % 4
    by_member = (to_lane == iota((512, 512), 1)).astype(BF16)
    parts = jnp.concatenate([p.astype(F32) for p in split3(g_ref[...])], axis=0).astype(BF16)
    given = jnp.dot(parts, by_member, preferred_element_type=F32)
    given = given[0:16] + given[16:32] + given[32:48]
    for m in range(8):
        piece = given[:, m * 64 : m * 64 + 64]
        page = jnp.concatenate([piece[0:8], piece[8:16]], axis=1)
        for copy in range(4):
            out_ref[m * 4 + copy] = page


def last_pairs(edge, hbm, q_parts, groups, notes, tasks, lanes, lane_rows, cols, fars, own_rows, extra):
    sizes, width = [h.shape[0] for h in hbm], hbm[0].shape[1]
    n_cols = tuple(len(c) for c in cols)
    small = lanes + [c for each in cols for c in each] + fars + [extra]
    return pl.pallas_call(
        functools.partial(
            last_kernel, tasks, q_parts, groups, len(hbm), lane_rows, n_cols, len(fars), own_rows
        ),
        out_shape=jax.ShapeDtypeStruct((32, 8, 128), F32),
        in_specs=[SMEM_SPEC] + [ANY_SPEC] * len(hbm) + [VMEM_SPEC] * (len(notes) + len(small)),
        out_specs=VMEM_SPEC,
        scratch_shapes=scratch_for(q_parts, groups, sizes, width)
        + [pltpu.VMEM((3, 512, 128), F32), pltpu.VMEM((3, 512, 128), F32), pltpu.VMEM((16, 512), F32)],
        cost_estimate=cost_of(tasks, q_parts, groups, sizes, width),
        compiler_params=LIMIT,
    )(edge.reshape(1), *hbm, *notes, *small)


def prep_kernel(pieces, own_ref, hit_ref, found_ref, half_ref, *refs):
    piece_refs, (buf, part, sems) = refs[: len(pieces)], refs[len(pieces) :]
    slab = 128
    n = buf.shape[0] // slab
    copies = [
        pltpu.make_async_copy(own_ref.at[i * slab : i * slab + slab, :], buf.at[i * slab : i * slab + slab, :], sems.at[i])
        for i in range(n)
    ]
    for copy in copies:
        copy.start()
    out = [
        pltpu.make_async_copy(buf.at[lo:hi, :], ref, sems.at[n + i])
        for i, ((lo, hi), ref) in enumerate(zip(pieces, piece_refs))
    ]
    for i, copy in enumerate(copies):
        copy.wait()
        for each, (lo, hi) in zip(out, pieces):
            if hi == i * slab + slab:
                each.start()

        def step(k, _, i=i):
            rows = pl.ds(pl.multiple_of(i * slab + k * 16, 16), 16)
            total = None
            for t in range(buf.shape[1] // 128):
                v = buf[rows, t * 128 : t * 128 + 128].astype(F32)
                total = v * v if total is None else total + v * v
            part[rows, :] = total
            return 0

        lax.fori_loop(0, slab // 16, step, 0)
    half_ref[...] = 0.5 * jnp.sum(jnp.transpose(part[...]), axis=0, keepdims=True)
    found = jnp.dot(hit_ref[...], buf[...], preferred_element_type=F32).astype(BF16)
    for i in range(8):
        found_ref[i] = found
    for each in out:
        each.wait()


def prepare(own, hit, pieces):
    width = own.shape[1]
    return pl.pallas_call(
        functools.partial(prep_kernel, pieces),
        out_shape=[jax.ShapeDtypeStruct((8, 8, width), BF16), jax.ShapeDtypeStruct((1, 512), F32)]
        + [jax.ShapeDtypeStruct((hi - lo, width), BF16) for lo, hi in pieces],
        in_specs=[ANY_SPEC, VMEM_SPEC],
        out_specs=[VMEM_SPEC, VMEM_SPEC] + [ANY_SPEC] * len(pieces),
        scratch_shapes=[
            pltpu.VMEM((512, width), BF16),
            pltpu.VMEM((512, 128), F32),
            pltpu.SemaphoreType.DMA((4 + len(pieces),)),
        ],
        cost_estimate=pl.CostEstimate(flops=2 * 512 * 512 * width, transcendentals=0, bytes_accessed=own.size * 2),
        compiler_params=LIMIT,
    )(own, hit)


def close_kernel(width, where_ref, in_ref, order_ref, keep_ref, total_ref, gain_ref, cover_ref):
    lane = iota((4, 128), 1)
    row = iota((4, 128), 0)

    def page(line, sd):
        return in_ref[where_ref[0] + where_ref[1] * (line % 4) + sd]

    final = jnp.zeros((8, 512), F32)
    far = jnp.zeros((1, 64), F32)
    half_sum = jnp.zeros((1, 64), F32)
    for line in range(4):
        for sd in range(2):
            here = page(line, sd)
            far = jnp.maximum(far, here[7:8, 0:64])
            half_sum = half_sum + here[3:4, 64:128]
            low = here[0:4] + jnp.where(row < 3, page(line + 1, sd)[4:8], 0.0)
            fourth = page(line, 0) if sd == 1 else page(line + 1, 1)
            high = jnp.where(row < 3, page(line + 3, sd)[0:4] + fourth[4:8], 0.0)
            both = jnp.where(lane < 64, low, high)
            both = both[:, 0:64] + both[:, 64:128]
            both = jnp.concatenate([both, jnp.zeros((4, 64), F32)], axis=0)
            at = (line * 2 + sd) * 64
            final = final + exact_dot(both, order_ref[at : at + 64, :])
    far = 2.0 * far[:, 0:1]
    half_sum = half_sum[:, 0:1]
    keep = keep_ref[...]
    total = total_ref[:, 0:1]
    scale = 1.0 / width
    gain_ref[0] = (2.0 * final[0:1] + total * far - 2.0 * half_sum) * scale * keep / total
    gain_ref[1] = 2.0 * final[1:2] * scale * keep / total
    gain_ref[2] = 2.0 * final[2:3] * scale * keep / total
    cover_ref[...] = keep * (far - 2.0 * final[3:4]) * scale


def source_of(x, z, y, core, row):
    group, sub, member, slot = row // 64, row // 32 % 2, row // 4 % 8, row % 4
    i, w = group // 4, group % 4
    outer = (y == 0) | (y == 3)
    low = y < 2
    y0 = jnp.where(outer, 3 * i, 1 + i)
    y1 = jnp.where(low, 1 - i, 2 + i)
    sx = jnp.where(core == 0, x, w)
    sz = jnp.where(core == 0, w, z)
    sy = jnp.where(core == 0, y0, y1)
    return dix(sx, sy, sz, jnp.where(sub == 0, 0, 1)), member, slot


def body(sketches, labels, places, counts, chosen):
    rows_dev, width = sketches.shape
    dp, cls = lax.axis_index("dp"), lax.axis_index("cls")
    x, zh, zl, y, core = dp // 2, dp % 2, cls // 8, cls // 2 % 4, cls % 2
    z = zh * 2 + zl
    edge = y % 2
    first = core == 0

    packed = jnp.concatenate([counts[0], jnp.broadcast_to(chosen, (3, 128))], axis=0)
    packed = send(packed, INFO)
    host_counts = packed[:8].astype(F32)
    picks = packed[8:11, 0]

    k_core, k_y, k_zl = labels % 2, labels // 2 % 4, labels // 8
    group = jnp.where(
        k_core == 0,
        (k_y // 2) * 4 + (k_y % 2) * 2 + k_zl,
        ((k_y + 3) % 4 // 2) * 4 + k_zl * 2 + k_y % 2,
    )
    spot = group * 64 + core * 32 + places // 512 * 4 + places % 4
    mine = jnp.where(k_core == core, spot, -1)
    theirs = jnp.where(k_core == core, -1, spot)
    from_twin = send(sketches, SWAP)
    twin_spot = send(theirs, SWAP)
    slots = iota((2 * rows_dev, rows_dev), 0)
    table_own = (slots == mine[None, :]).astype(BF16)
    table_twin = (slots == twin_spot[None, :]).astype(BF16)
    outgoing = (
        jnp.dot(table_own, sketches, preferred_element_type=F32)
        + jnp.dot(table_twin, from_twin, preferred_element_type=F32)
    ).astype(BF16)
    own = lax.all_to_all(
        outgoing.reshape(8, 64, width), AX, 0, 0, axis_index_groups=regroup_groups(), tiled=True
    ).reshape(512, width)

    src, member, slot = source_of(x, z, y, core, iota((1, 512), 1))
    place = member * 512 + src * 4 + slot
    seen = jnp.sum(
        jnp.where(iota((128, 512), 0) == src, exact(host_counts.T, (iota((8, 512), 0) == member).astype(F32)), 0.0),
        axis=0,
    )
    valid = slot[0].astype(F32) < seen
    n_valid = jnp.sum(host_counts)
    hit = (place == jnp.concatenate([picks, -jnp.ones((5,), jnp.int32)])[:, None]).astype(BF16)
    found, half, *cuts = prepare(own, hit, tuple((i, i + 128) for i in range(0, 512, 128)))
    half = half[0]

    l = [send(v, UP) for v in cuts]
    relays = [jnp.where(edge == 0, v, cut) for v, cut in zip(l, cuts)]
    f = [send(v, ACROSS) for v in relays]
    r = send(own, DOWN)

    found = lax.all_to_all(found, AX, 0, 0, axis_index_groups=class_groups(), tiled=True)
    found, _ = lax.optimization_barrier((found, relays[0]))
    found = jnp.sum(found.astype(F32), axis=0).astype(BF16)
    to_picks = inner(found, own)
    pick_half = 0.5 * jnp.sum(jnp.square(found.astype(F32)), axis=1)
    near = pick_half[:3, None] - to_picks[:3]
    near1 = near[0]
    near2 = jnp.minimum(near[0], near[1])
    near3 = jnp.minimum(near2, near[2])
    info = jnp.stack(
        [half, jnp.where(valid, half, -BIG), jnp.where(valid, near1, -BIG), jnp.where(valid, near2, -BIG)]
        + [jnp.zeros((512,), F32)] * 4
    )
    info_l = send(info, UP)
    info_r = send(info, DOWN)
    info_f = send(info, FOURTH)

    mid = 256
    l_low, l_high = info_l[:, :mid], info_l[:, mid:]
    f_low, f_high = info_f[:, :mid], info_f[:, mid:]
    lanes_1, _, far_1 = early_pairs(edge, [own], [[0]], [None], [info, info], [(0, [(0, True, False)])])
    lanes_2, cols_2, far_2 = early_pairs(
        edge,
        [own, l[0], l[1], f[0], f[1]],
        [[0]],
        [[1, 2], [3, 4]],
        [info, l_low, f_low],
        [(0, [(0, True, True)]), (1, [(0, True, True)])],
    )
    lanes_3, cols_3, far_3 = early_pairs(
        edge,
        [own, r, *l, f[0], f[1]],
        [[0], [1]],
        [[6, 7], [4, 5], [2, 3]],
        [info, info_r, f_low, l_high, l_low],
        [
            (2, [(1, False, True)]),
            (0, [(1, True, True)]),
            (1, [(0, True, True), (1, False, True)]),
        ],
    )
    none = jnp.zeros((512,), F32)
    extra = [none] * 16
    extra[0] = -n_valid * half
    extra[3] = half + near3
    extra[11] = jnp.broadcast_to(jnp.sum(half), (512,))
    extra = jnp.stack(extra)
    lane_list = [
        (lanes_1[0], (0, 0)),
        (lanes_2[0], (4, 0)),
        (lanes_2[1], (12, 0)),
        (lanes_3[0], (12, 0)),
        (lanes_3[1], (4, mid)),
    ]
    outbox = last_pairs(
        edge,
        [own, r, f[2], f[3]],
        [[0], [1]],
        [[2, 3]],
        [info, info_r, f_high],
        [(0, [(0, True, True), (1, True, True)])],
        [v for v, _ in lane_list],
        [at for _, at in lane_list],
        [[cols_2[0], cols_3[0]], [cols_3[1]]],
        [far_1, far_2, far_3],
        {0: (12, mid)},
        extra,
    )
    inbox = lax.all_to_all(outbox, AX, 0, 0, axis_index_groups=final_groups(), tiled=True)

    lane1 = iota((512, 1), 0)
    line, sd, rest = lane1 // 128, lane1 // 64 % 2, lane1 % 64
    pair_y0 = y // 2 * 2 + sd
    pair_low = (y == 1) | (y == 2)
    pair_y1 = jnp.where(pair_low, 2 - sd, 3 * sd)
    pair_y = jnp.where(first, pair_y0, pair_y1)
    src2, _, slot2 = source_of(line, line, pair_y, core, (rest // 4) * 32 + rest % 4)
    in_order = (src2 * 4 + slot2 == iota((512, 512), 1)).astype(F32)

    class_counts = counts[0]
    own_counts = lax.dynamic_index_in_dim(class_counts, dp, 0, keepdims=False)
    keep = (iota((128, 4), 1) < own_counts[:, None]).reshape(1, 512).astype(F32)
    total = jnp.broadcast_to(jnp.sum(class_counts).astype(F32), (1, 128))
    host = jnp.where(first, (edge * 2 + zl) * 2, (zl * 2 + edge) * 8)
    where = jnp.stack([host, jnp.where(first, 8, 2)])
    gains, cover = pl.pallas_call(
        functools.partial(close_kernel, width),
        out_shape=[jax.ShapeDtypeStruct((3, 1, 512), F32), jax.ShapeDtypeStruct((1, 512), F32)],
        in_specs=[pl.BlockSpec(memory_space=pltpu.SMEM)] + [VMEM_SPEC] * 4,
        out_specs=[VMEM_SPEC, VMEM_SPEC],
    )(where, inbox, in_order, keep, total)
    return (gains, cover)


def solution(mesh):
    placed = (
        P(("dp", "cls"), None),
        P(("dp", "cls")),
        P(("dp", "cls")),
        P("cls", None, None),
        P(None, "cls"),
    )
    return jax.shard_map(
        body,
        mesh=mesh,
        in_specs=placed,
        out_specs=(P(None, "cls", "dp"), P("cls", "dp")),
        check_vma=False,
    )
```

```python
import functools

import jax
import jax.numpy as jnp
from jax import lax
from jax.experimental import pallas as pl
from jax.experimental.pallas import tpu as pltpu
from jax.sharding import PartitionSpec as P


AX = ("dp", "cls")
F32 = jnp.float32
BF16 = jnp.bfloat16
BIG = 1e30
STEP = 64


def dix(x, y, z, c):
    return x * 32 + (z // 2) * 16 + (z % 2) * 8 + y * 2 + c


def xyz(d):
    return d // 32, (d // 2) % 4, ((d // 16) % 2) * 2 + (d // 8) % 2, d % 2


DEV = range(128)
MATE = ((1, 0, 3, 2), (3, 2, 1, 0))
PAIRS = (((0, 1), (2, 3)), ((2, 1), (0, 3)))


def mate(d):
    x, y, z, c = xyz(d)
    return dix(x, MATE[c][y], z, c)


def along(d, k):
    x, y, z, c = xyz(d)
    return dix((x + k) % 4, y, z, c) if c == 0 else dix(x, y, (z + k) % 4, c)


def side(d):
    return xyz(d)[1] % 2


SWAP = [(d, d ^ 1) for d in DEV]
UP = [(d, along(d, 1)) for d in DEV]
DOWN = [(d, along(d, -1)) for d in DEV]
ACROSS = [(d, mate(d)) for d in DEV]
FOURTH = [(d, mate(d) if side(d) == 1 else mate(along(d, 1))) for d in DEV]


def regroup_groups():
    groups = []
    for x in range(4):
        for ys in ((0, 3), (1, 2)):
            groups.append([dix(x, y, z, 0) for y in ys for z in range(4)])
    for z in range(4):
        for ys in ((1, 0), (2, 3)):
            groups.append([dix(x, y, z, 1) for y in ys for x in range(4)])
    return groups


def class_groups():
    groups = []
    for c in (0, 1):
        for pair in PAIRS[c]:
            for u in range(4):
                group = [dix(t, y, u, 0) if c == 0 else dix(u, y, t, 1) for t in range(4) for y in pair]
                groups.append(group)
    return groups


def final_groups():
    groups = []
    for c in (0, 1):
        for pair in PAIRS[c]:
            groups.append([dix(x, y, z, c) for x in range(4) for z in range(4) for y in pair])
    return groups


def info_pairs():
    out = []
    for d in DEV:
        x, y, z, c = xyz(d)
        zh, zl = z // 2, z % 2
        if c == 0:
            src = dix(x, (y // 2) * 2 + zh, (y % 2) * 2 + zl, 0)
        else:
            yk = y if y % 2 == x % 2 else MATE[1][y]
            src = dix(zh * 2 + zl, yk, (y % 2) * 2 + x // 2, 1)
        out.append((src, d))
    return out


INFO = info_pairs()


def send(value, pairs):
    return lax.ppermute(value, AX, pairs)


def iota(shape, dim):
    return lax.broadcasted_iota(jnp.int32, shape, dim)


def inner(left, right):
    return lax.dot_general(left, right, (((1,), (1,)), ((), ())), preferred_element_type=F32)


def exact(left, right):
    return jnp.dot(left, right, precision=lax.Precision.HIGHEST, preferred_element_type=F32)


def split3(value):
    high = value.astype(BF16)
    rest = value - high.astype(F32)
    middle = rest.astype(BF16)
    return high, middle, (rest - middle.astype(F32)).astype(BF16)


def pair_work(side, tasks, q_parts, groups, hbm, note_refs, col_refs, q_buf, u_bufs, x_ref, side_ref, sems):
    copies = {}
    count = 0
    for kind, parts, bufs in (("q", q_parts, [q_buf] * len(q_parts)), ("u", groups, u_bufs)):
        for i, members in enumerate(parts):
            if members is None:
                continue
            at = i * 512 if kind == "q" else 0
            for member in members:
                either = isinstance(member, tuple)
                k = hbm[member[2] if either else member].shape[0]
                target = bufs[i].at[at : at + k, :]
                if either:
                    one = pltpu.make_async_copy(hbm[member[0]].at[member[1] : member[1] + k, :], target, sems.at[count])
                    two = pltpu.make_async_copy(hbm[member[2]], target, sems.at[count])
                    copies.setdefault((kind, i), []).append((one, two))
                else:
                    copies.setdefault((kind, i), []).append((pltpu.make_async_copy(hbm[member], target, sems.at[count]),))
                count += 1
                at += k
    begun = []
    for g, rows in tasks:
        for key in [("u", g)] + [("q", q) for q, _, _ in rows]:
            if key in copies and key not in begun:
                begun.append(key)
                for copy in copies[key]:
                    if len(copy) == 1:
                        copy[0].start()
                    else:
                        for choice in (0, 1):
                            pl.when(side == choice)(copy[choice].start)
    for q in range(len(q_parts)):
        parts = jnp.concatenate([p.astype(F32) for p in split3(note_refs[q][...])], axis=0).astype(BF16)
        along = (iota((24, 512), 0) % 8 == iota((24, 512), 1) // 128).astype(BF16)
        wide = lax.dot_general(parts, along, (((0,), (0,)), ((), ())), preferred_element_type=F32)
        for j in range(4):
            side_ref[q, j] = wide[:, j * 128 : j * 128 + 128]
    ready = set()
    fresh = set(col_refs)
    far = jnp.zeros((8, 128), F32)
    lanes = {}
    for g, given in tasks:
        data = q_buf if groups[g] is None else u_bufs[g]
        m = 512 if groups[g] is None else data.shape[0]
        lo, hi = 512 * given[0][0], 512 * given[-1][0] + 512
        tiles = m // 128
        u_half, u_mark, u_one, u_two = [
            [
                jnp.broadcast_to(note_refs[len(q_parts) + g][i : i + 1, t * 128 : t * 128 + 128], (8, 128))
                for t in range(tiles)
            ]
            for i in range(4)
        ]
        for key in [("u", g)] + [("q", q) for q, _, _ in given]:
            if key in copies and key not in ready:
                ready.add(key)
                for copy in copies[key]:
                    copy[0].wait()
        x_ref[lo:hi, :m] = lax.dot_general(
            q_buf[lo:hi], data[:m], (((1,), (1,)), ((), ())), preferred_element_type=F32
        )
        for q, to_u, to_q in given:
            first_use = to_q and q in fresh
            if to_q:
                fresh.discard(q)

            def step(i, carry, q=q, to_u=to_u, to_q=to_q, first_use=first_use, tiles=tiles, u=(u_half, u_mark, u_one, u_two)):
                carry = [list(c) for c in carry]
                u_half, u_mark, u_one, u_two = u
                start = pl.multiple_of(i * STEP, STEP)
                for k in range(STEP // 8):
                    rows = pl.ds(start + k * 8, 8)
                    q_half, q_mark, q_one, q_two = (side_ref[q, j, rows, :] for j in range(4))
                    sums = [None, None, None]
                    for t in range(tiles):
                        x = x_ref[pl.ds(start + (q * 512 + k * 8), 8), t * 128 : t * 128 + 128]
                        carry[0][t] = jnp.maximum(carry[0][t], (q_mark - x) + u_mark[t])
                        if to_u:
                            carry[1][t] = carry[1][t] + x
                            carry[2][t] = carry[2][t] + jnp.maximum((x + q_one) - u_half[t], 0.0)
                            carry[3][t] = carry[3][t] + jnp.maximum((x + q_two) - u_half[t], 0.0)
                        if to_q:
                            off = x - q_half
                            values = (x, jnp.maximum(off + u_one[t], 0.0), jnp.maximum(off + u_two[t], 0.0))
                            sums = [v if s is None else s + v for s, v in zip(sums, values)]
                    if to_q:
                        for j in range(3):
                            if first_use:
                                col_refs[q][j, rows, :] = sums[j]
                            else:
                                col_refs[q][j, rows, :] += sums[j]
                return carry

            zero = [jnp.zeros((8, 128), F32)] * tiles
            done = lax.fori_loop(0, 512 // STEP, step, [zero] * (4 if to_u else 1))
            for t in range(tiles):
                far = jnp.maximum(far, done[0][t])
            if to_u:
                done = done[1:]
                lanes[g] = [[a + b for a, b in zip(v, w)] for v, w in zip(lanes[g], done)] if g in lanes else done
    rows = {
        g: [
            jnp.concatenate([jnp.sum(v, axis=0, keepdims=True) for v in kind], axis=1) for kind in value
        ]
        for g, value in lanes.items()
    }
    return rows, far


def rows_of(part, sizes):
    return sum(sizes[i[2] if isinstance(i, tuple) else i] for i in part)


def scratch_for(q_parts, groups, sizes, width):
    q_bufs = [pltpu.VMEM((512 * len(q_parts), width), BF16)]
    u_sizes = [rows_of(p, sizes) if p else 0 for p in groups]
    u_bufs = [pltpu.VMEM((n or 16, width), BF16) for n in u_sizes]
    n_copies = sum(len(p) for p in q_parts) + sum(len(p) for p in groups if p)
    most = max([n or 512 for n in u_sizes])
    return q_bufs + u_bufs + [
        pltpu.VMEM((512 * len(q_parts), most), F32),
        pltpu.VMEM((len(q_parts), 4, 512, 128), F32),
        pltpu.SemaphoreType.DMA((n_copies,)),
    ]


def cost_of(tasks, q_parts, groups, sizes, width):
    def rows(p):
        return rows_of(p or q_parts[0], sizes)

    flops = sum(2 * 512 * len(t[1]) * rows(groups[t[0]]) * width for t in tasks)
    moved = 2 * width * sum(sizes)
    return pl.CostEstimate(flops=flops, transcendentals=0, bytes_accessed=moved)


VMEM_SPEC = pl.BlockSpec(memory_space=pltpu.VMEM)
SMEM_SPEC = pl.BlockSpec(memory_space=pltpu.SMEM)
ANY_SPEC = pl.BlockSpec(memory_space=pltpu.HBM)
LIMIT = pltpu.CompilerParams(vmem_limit_bytes=36 * 2**20)


def early_kernel(tasks, q_parts, groups, n_hbm, lane_outs, col_outs, side_ref_in, *refs):
    hbm, refs = refs[:n_hbm], refs[n_hbm:]
    n_notes = len(q_parts) + len(groups)
    notes, refs = refs[:n_notes], refs[n_notes:]
    lane_refs, refs = refs[: len(lane_outs)], refs[len(lane_outs) :]
    cols, refs = dict(zip(col_outs, refs)), refs[len(col_outs) :]
    far_ref, refs = refs[0], refs[1:]
    q_buf, refs = refs[0], refs[1:]
    u_bufs, (x_ref, side_ref, sems) = refs[: len(groups)], refs[len(groups) :]
    rows, far = pair_work(side_ref_in[0], tasks, q_parts, groups, hbm, notes, cols, q_buf, u_bufs, x_ref, side_ref, sems)
    for g, ref in zip(lane_outs, lane_refs):
        ref[...] = jnp.zeros_like(ref)
        for j in range(3):
            ref[j : j + 1, :] = rows[g][j]
    far_ref[...] = far


def early_pairs(edge, hbm, q_parts, groups, notes, tasks):
    sizes, width = [h.shape[0] for h in hbm], hbm[0].shape[1]
    lane_outs = [t[0] for t in tasks if any(v[1] for v in t[1])]
    col_outs = [q for q in range(len(q_parts)) if any(v[0] == q and v[2] for t in tasks for v in t[1])]
    shapes = [jax.ShapeDtypeStruct((8, notes[len(q_parts) + g].shape[1]), F32) for g in lane_outs]
    shapes += [jax.ShapeDtypeStruct((3, 512, 128), F32) for _ in col_outs]
    shapes += [jax.ShapeDtypeStruct((8, 128), F32)]
    out = pl.pallas_call(
        functools.partial(early_kernel, tasks, q_parts, groups, len(hbm), lane_outs, col_outs),
        out_shape=shapes,
        in_specs=[SMEM_SPEC] + [ANY_SPEC] * len(hbm) + [VMEM_SPEC] * len(notes),
        out_specs=[VMEM_SPEC] * len(shapes),
        scratch_shapes=scratch_for(q_parts, groups, sizes, width),
        cost_estimate=cost_of(tasks, q_parts, groups, sizes, width),
        compiler_params=LIMIT,
    )(edge.reshape(1), *hbm, *notes)
    n = len(lane_outs)
    return dict(zip(lane_outs, out)), dict(zip(col_outs, out[n:])), out[-1]


def last_kernel(tasks, q_parts, groups, n_hbm, lane_rows, n_cols, n_far, own_rows, side_ref_in, *refs):
    hbm, refs = refs[:n_hbm], refs[n_hbm:]
    n_notes = len(q_parts) + len(groups)
    notes, refs = refs[:n_notes], refs[n_notes:]
    lane_refs, refs = refs[: len(lane_rows)], refs[len(lane_rows) :]
    col_refs, refs = refs[: sum(n_cols)], refs[sum(n_cols) :]
    far_refs, refs = refs[:n_far], refs[n_far:]
    extra_ref, out_ref, refs = refs[0], refs[1], refs[2:]
    q_buf, refs = refs[0], refs[1:]
    u_bufs, refs = refs[: len(groups)], refs[len(groups) :]
    x_ref, side_ref, sems, col0_ref, col1_ref, g_ref = refs
    cols = {0: col0_ref, 1: col1_ref}
    rows, far = pair_work(side_ref_in[0], tasks, q_parts, groups, hbm, notes, cols, q_buf, u_bufs, x_ref, side_ref, sems)
    g_ref[...] = extra_ref[...]
    for ref, (row, at) in zip(lane_refs, lane_rows):
        m = ref.shape[1]
        g_ref[row : row + 3, at : at + m] += ref[0:3, :]
    for g, (row, at) in own_rows.items():
        for j in range(3):
            value = rows[g][j]
            g_ref[row + j : row + j + 1, at : at + value.shape[1]] += value
    start = 0
    for q, (n, row) in enumerate(zip(n_cols, (0, 8))):
        for j in range(3):
            total = cols[q][j]
            for ref in col_refs[start : start + n]:
                total = total + ref[j]
            across = jnp.sum(jnp.transpose(total), axis=0, keepdims=True)
            g_ref[row + j : row + j + 1, :] += across
        start += n
    for ref in far_refs:
        far = jnp.maximum(far, ref[...])
    far = jnp.max(jnp.max(far, axis=0, keepdims=True), axis=1, keepdims=True)
    g_ref[7:8, :] = jnp.broadcast_to(far, (1, 512))
    lane = iota((512, 512), 0)
    to_lane = (lane // 4 % 8) * 64 + (lane // 32) * 4 + lane % 4
    by_member = (to_lane == iota((512, 512), 1)).astype(BF16)
    parts = jnp.concatenate([p.astype(F32) for p in split3(g_ref[...])], axis=0).astype(BF16)
    given = jnp.dot(parts, by_member, preferred_element_type=F32)
    given = given[0:16] + given[16:32] + given[32:48]
    for m in range(8):
        piece = given[:, m * 64 : m * 64 + 64]
        page = jnp.concatenate([piece[0:8], piece[8:16]], axis=1)
        for copy in range(4):
            out_ref[m * 4 + copy] = page


def last_pairs(edge, hbm, q_parts, groups, notes, tasks, lanes, lane_rows, cols, fars, own_rows, extra):
    sizes, width = [h.shape[0] for h in hbm], hbm[0].shape[1]
    n_cols = tuple(len(c) for c in cols)
    small = lanes + [c for each in cols for c in each] + fars + [extra]
    return pl.pallas_call(
        functools.partial(
            last_kernel, tasks, q_parts, groups, len(hbm), lane_rows, n_cols, len(fars), own_rows
        ),
        out_shape=jax.ShapeDtypeStruct((32, 8, 128), F32),
        in_specs=[SMEM_SPEC] + [ANY_SPEC] * len(hbm) + [VMEM_SPEC] * (len(notes) + len(small)),
        out_specs=VMEM_SPEC,
        scratch_shapes=scratch_for(q_parts, groups, sizes, width)
        + [pltpu.VMEM((3, 512, 128), F32), pltpu.VMEM((3, 512, 128), F32), pltpu.VMEM((16, 512), F32)],
        cost_estimate=cost_of(tasks, q_parts, groups, sizes, width),
        compiler_params=LIMIT,
    )(edge.reshape(1), *hbm, *notes, *small)


def prep_kernel(pieces, own_ref, hit_ref, found_ref, half_ref, *refs):
    piece_refs, (buf, part, sems) = refs[: len(pieces)], refs[len(pieces) :]
    slab = 128
    n = buf.shape[0] // slab
    copies = [
        pltpu.make_async_copy(own_ref.at[i * slab : i * slab + slab, :], buf.at[i * slab : i * slab + slab, :], sems.at[i])
        for i in range(n)
    ]
    for copy in copies:
        copy.start()
    out = [
        pltpu.make_async_copy(buf.at[lo:hi, :], ref, sems.at[n + i])
        for i, ((lo, hi), ref) in enumerate(zip(pieces, piece_refs))
    ]
    for i, copy in enumerate(copies):
        copy.wait()
        for each, (lo, hi) in zip(out, pieces):
            if hi == i * slab + slab:
                each.start()

        def step(k, _, i=i):
            rows = pl.ds(pl.multiple_of(i * slab + k * 16, 16), 16)
            total = None
            for t in range(buf.shape[1] // 128):
                v = buf[rows, t * 128 : t * 128 + 128].astype(F32)
                total = v * v if total is None else total + v * v
            part[rows, :] = total
            return 0

        lax.fori_loop(0, slab // 16, step, 0)
    half_ref[...] = 0.5 * jnp.sum(jnp.transpose(part[...]), axis=0, keepdims=True)
    found = jnp.dot(hit_ref[...], buf[...], preferred_element_type=F32).astype(BF16)
    for i in range(8):
        found_ref[i] = found
    for each in out:
        each.wait()


def prepare(own, hit, pieces):
    width = own.shape[1]
    return pl.pallas_call(
        functools.partial(prep_kernel, pieces),
        out_shape=[jax.ShapeDtypeStruct((8, 8, width), BF16), jax.ShapeDtypeStruct((1, 512), F32)]
        + [jax.ShapeDtypeStruct((hi - lo, width), BF16) for lo, hi in pieces],
        in_specs=[ANY_SPEC, VMEM_SPEC],
        out_specs=[VMEM_SPEC] * 3 + [ANY_SPEC] * (len(pieces) - 1),
        scratch_shapes=[
            pltpu.VMEM((512, width), BF16),
            pltpu.VMEM((512, 128), F32),
            pltpu.SemaphoreType.DMA((4 + len(pieces),)),
        ],
        cost_estimate=pl.CostEstimate(flops=2 * 512 * 512 * width, transcendentals=0, bytes_accessed=own.size * 2),
        compiler_params=LIMIT,
    )(own, hit)


def close_kernel(width, where_ref, in_ref, order_ref, keep_ref, total_ref, gain_ref, cover_ref):
    lane = iota((4, 128), 1)
    row = iota((4, 128), 0)

    def page(line, sd):
        return in_ref[where_ref[0] + where_ref[1] * (line % 4) + sd]

    final = jnp.zeros((8, 512), F32)
    far = jnp.zeros((1, 64), F32)
    half_sum = jnp.zeros((1, 64), F32)
    for line in range(4):
        for sd in range(2):
            here = page(line, sd)
            far = jnp.maximum(far, here[7:8, 0:64])
            half_sum = half_sum + here[3:4, 64:128]
            low = here[0:4] + jnp.where(row < 3, page(line + 1, sd)[4:8], 0.0)
            fourth = page(line, 0) if sd == 1 else page(line + 1, 1)
            high = jnp.where(row < 3, page(line + 3, sd)[0:4] + fourth[4:8], 0.0)
            both = jnp.where(lane < 64, low, high)
            both = both[:, 0:64] + both[:, 64:128]
            both = jnp.concatenate([both, jnp.zeros((4, 64), F32)], axis=0)
            at = (line * 2 + sd) * 64
            parts = jnp.concatenate([p.astype(F32) for p in split3(both)], axis=0).astype(BF16)
            moved = jnp.dot(parts, order_ref[at : at + 64, :], preferred_element_type=F32)
            final = final + (moved[0:8] + moved[8:16] + moved[16:24])
    far = 2.0 * far[:, 0:1]
    half_sum = half_sum[:, 0:1]
    keep = keep_ref[...]
    total = total_ref[:, 0:1]
    scale = 1.0 / width
    gain_ref[0] = (2.0 * final[0:1] + total * far - 2.0 * half_sum) * scale * keep / total
    gain_ref[1] = 2.0 * final[1:2] * scale * keep / total
    gain_ref[2] = 2.0 * final[2:3] * scale * keep / total
    cover_ref[...] = keep * (far - 2.0 * final[3:4]) * scale


def source_of(x, z, y, core, row):
    group, sub, member, slot = row // 64, row // 32 % 2, row // 4 % 8, row % 4
    i, w = group // 4, group % 4
    outer = (y == 0) | (y == 3)
    low = y < 2
    y0 = jnp.where(outer, 3 * i, 1 + i)
    y1 = jnp.where(low, 1 - i, 2 + i)
    sx = jnp.where(core == 0, x, w)
    sz = jnp.where(core == 0, w, z)
    sy = jnp.where(core == 0, y0, y1)
    return dix(sx, sy, sz, jnp.where(sub == 0, 0, 1)), member, slot


def body(sketches, labels, places, counts, chosen):
    rows_dev, width = sketches.shape
    dp, cls = lax.axis_index("dp"), lax.axis_index("cls")
    x, zh, zl, y, core = dp // 2, dp % 2, cls // 8, cls // 2 % 4, cls % 2
    z = zh * 2 + zl
    edge = y % 2
    first = core == 0

    packed = jnp.concatenate([counts[0], jnp.broadcast_to(chosen, (3, 128))], axis=0)
    packed = send(packed, INFO)
    host_counts = packed[:8].astype(F32)
    picks = packed[8:11, 0]

    k_core, k_y, k_zl = labels % 2, labels // 2 % 4, labels // 8
    group = jnp.where(
        k_core == 0,
        (k_y // 2) * 4 + (k_y % 2) * 2 + k_zl,
        ((k_y + 3) % 4 // 2) * 4 + k_zl * 2 + k_y % 2,
    )
    spot = group * 64 + core * 32 + places // 512 * 4 + places % 4
    mine = jnp.where(k_core == core, spot, -1)
    theirs = jnp.where(k_core == core, -1, spot)
    from_twin = send(sketches, SWAP)
    twin_spot = send(theirs, SWAP)
    slots = iota((2 * rows_dev, rows_dev), 0)
    table_own = (slots == mine[None, :]).astype(BF16)
    table_twin = (slots == twin_spot[None, :]).astype(BF16)
    outgoing = (
        jnp.dot(table_own, sketches, preferred_element_type=F32)
        + jnp.dot(table_twin, from_twin, preferred_element_type=F32)
    ).astype(BF16)
    own = lax.all_to_all(
        outgoing.reshape(8, 64, width), AX, 0, 0, axis_index_groups=regroup_groups(), tiled=True
    ).reshape(512, width)

    src, member, slot = source_of(x, z, y, core, iota((1, 512), 1))
    place = member * 512 + src * 4 + slot
    seen = jnp.sum(
        jnp.where(iota((128, 512), 0) == src, exact(host_counts.T, (iota((8, 512), 0) == member).astype(F32)), 0.0),
        axis=0,
    )
    valid = slot[0].astype(F32) < seen
    n_valid = jnp.sum(host_counts)
    hit = (place == jnp.concatenate([picks, -jnp.ones((5,), jnp.int32)])[:, None]).astype(BF16)
    found, half, *cuts = prepare(own, hit, tuple((i, i + 128) for i in range(0, 512, 128)))
    half = half[0]

    l = [send(v, UP) for v in cuts]
    first_relay = jnp.where(edge == 0, l[0], cuts[0])
    r = send(own, DOWN)

    found = lax.all_to_all(found, AX, 0, 0, axis_index_groups=class_groups(), tiled=True)
    found, _ = lax.optimization_barrier((found, first_relay))
    found = jnp.sum(found.astype(F32), axis=0).astype(BF16)
    to_picks = inner(found, own)
    second, to_picks = lax.optimization_barrier((l[1], to_picks))
    relays = [first_relay] + [jnp.where(edge == 0, v, cut) for v, cut in zip([second, *l[2:]], cuts[1:])]
    f = [send(v, ACROSS) for v in relays]
    pick_half = 0.5 * jnp.sum(jnp.square(found.astype(F32)), axis=1)
    near = pick_half[:3, None] - to_picks[:3]
    near1 = near[0]
    near2 = jnp.minimum(near[0], near[1])
    near3 = jnp.minimum(near2, near[2])
    info = jnp.stack(
        [half, jnp.where(valid, half, -BIG), jnp.where(valid, near1, -BIG), jnp.where(valid, near2, -BIG)]
        + [jnp.zeros((512,), F32)] * 4
    )
    info_l = send(info, UP)
    info_r = send(info, DOWN)
    info_f = send(info, FOURTH)

    mid = 256
    l_low, l_high = info_l[:, :mid], info_l[:, mid:]
    f_low, f_high = info_f[:, :mid], info_f[:, mid:]
    lanes_1, _, far_1 = early_pairs(edge, [own], [[0]], [None], [info, info], [(0, [(0, True, False)])])
    lanes_2, cols_2, far_2 = early_pairs(
        edge,
        [own, l[0], l[1], f[0], f[1]],
        [[0]],
        [[1, 2], [3, 4]],
        [info, l_low, f_low],
        [(0, [(0, True, True)]), (1, [(0, True, True)])],
    )
    lanes_3, cols_3, far_3 = early_pairs(
        edge,
        [own, r, *l, f[0], f[1]],
        [[0], [1]],
        [[6, 7], [4, 5], [2, 3]],
        [info, info_r, f_low, l_high, l_low],
        [
            (2, [(1, False, True)]),
            (0, [(1, True, True)]),
            (1, [(0, True, True), (1, False, True)]),
        ],
    )
    none = jnp.zeros((512,), F32)
    extra = [none] * 16
    extra[0] = -n_valid * half
    extra[3] = half + near3
    extra[11] = jnp.broadcast_to(jnp.sum(half), (512,))
    extra = jnp.stack(extra)
    lane_list = [
        (lanes_1[0], (0, 0)),
        (lanes_2[0], (4, 0)),
        (lanes_2[1], (12, 0)),
        (lanes_3[0], (12, 0)),
        (lanes_3[1], (4, mid)),
    ]
    outbox = last_pairs(
        edge,
        [own, r, f[2], f[3]],
        [[0], [1]],
        [[2, 3]],
        [info, info_r, f_high],
        [(0, [(0, True, True), (1, True, True)])],
        [v for v, _ in lane_list],
        [at for _, at in lane_list],
        [[cols_2[0], cols_3[0]], [cols_3[1]]],
        [far_1, far_2, far_3],
        {0: (12, mid)},
        extra,
    )
    inbox = lax.all_to_all(outbox, AX, 0, 0, axis_index_groups=final_groups(), tiled=True)

    lane1 = iota((512, 1), 0)
    line, sd, rest = lane1 // 128, lane1 // 64 % 2, lane1 % 64
    pair_y0 = y // 2 * 2 + sd
    pair_low = (y == 1) | (y == 2)
    pair_y1 = jnp.where(pair_low, 2 - sd, 3 * sd)
    pair_y = jnp.where(first, pair_y0, pair_y1)
    src2, _, slot2 = source_of(line, line, pair_y, core, (rest // 4) * 32 + rest % 4)
    in_order = (src2 * 4 + slot2 == iota((512, 512), 1)).astype(BF16)

    class_counts = counts[0]
    own_counts = lax.dynamic_index_in_dim(class_counts, dp, 0, keepdims=False)
    keep = (iota((128, 4), 1) < own_counts[:, None]).reshape(1, 512).astype(F32)
    total = jnp.broadcast_to(jnp.sum(class_counts).astype(F32), (1, 128))
    host = jnp.where(first, (edge * 2 + zl) * 2, (zl * 2 + edge) * 8)
    where = jnp.stack([host, jnp.where(first, 8, 2)])
    gains, cover = pl.pallas_call(
        functools.partial(close_kernel, width),
        out_shape=[jax.ShapeDtypeStruct((3, 1, 512), F32), jax.ShapeDtypeStruct((1, 512), F32)],
        in_specs=[pl.BlockSpec(memory_space=pltpu.SMEM)] + [VMEM_SPEC] * 4,
        out_specs=[VMEM_SPEC, VMEM_SPEC],
    )(where, inbox, in_order, keep, total)
    return (gains, cover)


def solution(mesh):
    placed = (
        P(("dp", "cls"), None),
        P(("dp", "cls")),
        P(("dp", "cls")),
        P("cls", None, None),
        P(None, "cls"),
    )
    return jax.shard_map(
        body,
        mesh=mesh,
        in_specs=placed,
        out_specs=(P(None, "cls", "dp"), P("cls", "dp")),
        check_vma=False,
    )
```

```python
import functools

import jax
import jax.numpy as jnp
from jax import lax
from jax.experimental import pallas as pl
from jax.experimental.pallas import tpu as pltpu
from jax.sharding import PartitionSpec as P


AX = ("dp", "cls")
F32 = jnp.float32
BF16 = jnp.bfloat16
BIG = 1e30
STEP = 64


def dix(x, y, z, c):
    return x * 32 + (z // 2) * 16 + (z % 2) * 8 + y * 2 + c


def xyz(d):
    return d // 32, (d // 2) % 4, ((d // 16) % 2) * 2 + (d // 8) % 2, d % 2


DEV = range(128)
MATE = ((1, 0, 3, 2), (3, 2, 1, 0))
PAIRS = (((0, 1), (2, 3)), ((2, 1), (0, 3)))


def mate(d):
    x, y, z, c = xyz(d)
    return dix(x, MATE[c][y], z, c)


def along(d, k):
    x, y, z, c = xyz(d)
    return dix((x + k) % 4, y, z, c) if c == 0 else dix(x, y, (z + k) % 4, c)


def side(d):
    return xyz(d)[1] % 2


SWAP = [(d, d ^ 1) for d in DEV]
UP = [(d, along(d, 1)) for d in DEV]
DOWN = [(d, along(d, -1)) for d in DEV]
ACROSS = [(d, mate(d)) for d in DEV]
FOURTH = [(d, mate(d) if side(d) == 1 else mate(along(d, 1))) for d in DEV]


def regroup_groups():
    groups = []
    for x in range(4):
        for ys in ((0, 3), (1, 2)):
            groups.append([dix(x, y, z, 0) for y in ys for z in range(4)])
    for z in range(4):
        for ys in ((1, 0), (2, 3)):
            groups.append([dix(x, y, z, 1) for y in ys for x in range(4)])
    return groups


def class_groups():
    groups = []
    for c in (0, 1):
        for pair in PAIRS[c]:
            for u in range(4):
                group = [dix(t, y, u, 0) if c == 0 else dix(u, y, t, 1) for t in range(4) for y in pair]
                groups.append(group)
    return groups


def final_groups():
    groups = []
    for c in (0, 1):
        for pair in PAIRS[c]:
            groups.append([dix(x, y, z, c) for x in range(4) for z in range(4) for y in pair])
    return groups


def info_pairs():
    out = []
    for d in DEV:
        x, y, z, c = xyz(d)
        zh, zl = z // 2, z % 2
        if c == 0:
            src = dix(x, (y // 2) * 2 + zh, (y % 2) * 2 + zl, 0)
        else:
            yk = y if y % 2 == x % 2 else MATE[1][y]
            src = dix(zh * 2 + zl, yk, (y % 2) * 2 + x // 2, 1)
        out.append((src, d))
    return out


INFO = info_pairs()


def send(value, pairs):
    return lax.ppermute(value, AX, pairs)


def iota(shape, dim):
    return lax.broadcasted_iota(jnp.int32, shape, dim)


def inner(left, right):
    return lax.dot_general(left, right, (((1,), (1,)), ((), ())), preferred_element_type=F32)


def exact(left, right):
    return jnp.dot(left, right, precision=lax.Precision.HIGHEST, preferred_element_type=F32)


def split3(value):
    high = value.astype(BF16)
    rest = value - high.astype(F32)
    middle = rest.astype(BF16)
    return high, middle, (rest - middle.astype(F32)).astype(BF16)


def pair_work(side, tasks, q_parts, groups, hbm, note_refs, col_refs, q_buf, u_bufs, x_ref, side_ref, sems):
    copies = {}
    count = 0
    for kind, parts, bufs in (("q", q_parts, [q_buf] * len(q_parts)), ("u", groups, u_bufs)):
        for i, members in enumerate(parts):
            if members is None:
                continue
            at = i * 512 if kind == "q" else 0
            for member in members:
                either = isinstance(member, tuple)
                k = hbm[member[2] if either else member].shape[0]
                target = bufs[i].at[at : at + k, :]
                if either:
                    one = pltpu.make_async_copy(hbm[member[0]].at[member[1] : member[1] + k, :], target, sems.at[count])
                    two = pltpu.make_async_copy(hbm[member[2]], target, sems.at[count])
                    copies.setdefault((kind, i), []).append((one, two))
                else:
                    copies.setdefault((kind, i), []).append((pltpu.make_async_copy(hbm[member], target, sems.at[count]),))
                count += 1
                at += k
    begun = []
    for g, rows in tasks:
        for key in [("u", g)] + [("q", q) for q, _, _ in rows]:
            if key in copies and key not in begun:
                begun.append(key)
                for copy in copies[key]:
                    if len(copy) == 1:
                        copy[0].start()
                    else:
                        for choice in (0, 1):
                            pl.when(side == choice)(copy[choice].start)
    for q in range(len(q_parts)):
        parts = jnp.concatenate([p.astype(F32) for p in split3(note_refs[q][...])], axis=0).astype(BF16)
        along = (iota((24, 512), 0) % 8 == iota((24, 512), 1) // 128).astype(BF16)
        wide = lax.dot_general(parts, along, (((0,), (0,)), ((), ())), preferred_element_type=F32)
        for j in range(4):
            side_ref[q, j] = wide[:, j * 128 : j * 128 + 128]
    ready = set()
    fresh = set(col_refs)
    far = jnp.zeros((8, 128), F32)
    lanes = {}
    for g, given in tasks:
        data = q_buf if groups[g] is None else u_bufs[g]
        m = 512 if groups[g] is None else data.shape[0]
        lo, hi = 512 * given[0][0], 512 * given[-1][0] + 512
        tiles = m // 128
        u_half, u_mark, u_one, u_two = [
            [
                jnp.broadcast_to(note_refs[len(q_parts) + g][i : i + 1, t * 128 : t * 128 + 128], (8, 128))
                for t in range(tiles)
            ]
            for i in range(4)
        ]
        for key in [("u", g)] + [("q", q) for q, _, _ in given]:
            if key in copies and key not in ready:
                ready.add(key)
                for copy in copies[key]:
                    copy[0].wait()
        x_ref[lo:hi, :m] = lax.dot_general(
            q_buf[lo:hi], data[:m], (((1,), (1,)), ((), ())), preferred_element_type=F32
        )
        for q, to_u, to_q in given:
            first_use = to_q and q in fresh
            if to_q:
                fresh.discard(q)

            def step(i, carry, q=q, to_u=to_u, to_q=to_q, first_use=first_use, tiles=tiles, u=(u_half, u_mark, u_one, u_two)):
                carry = [list(c) for c in carry]
                u_half, u_mark, u_one, u_two = u
                start = pl.multiple_of(i * STEP, STEP)
                for k in range(STEP // 8):
                    rows = pl.ds(start + k * 8, 8)
                    q_half, q_mark, q_one, q_two = (side_ref[q, j, rows, :] for j in range(4))
                    sums = [None, None, None]
                    for t in range(tiles):
                        x = x_ref[pl.ds(start + (q * 512 + k * 8), 8), t * 128 : t * 128 + 128]
                        carry[0][t] = jnp.maximum(carry[0][t], (q_mark - x) + u_mark[t])
                        if to_u:
                            carry[1][t] = carry[1][t] + x
                            carry[2][t] = carry[2][t] + jnp.maximum((x + q_one) - u_half[t], 0.0)
                            carry[3][t] = carry[3][t] + jnp.maximum((x + q_two) - u_half[t], 0.0)
                        if to_q:
                            off = x - q_half
                            values = (x, jnp.maximum(off + u_one[t], 0.0), jnp.maximum(off + u_two[t], 0.0))
                            sums = [v if s is None else s + v for s, v in zip(sums, values)]
                    if to_q:
                        for j in range(3):
                            if first_use:
                                col_refs[q][j, rows, :] = sums[j]
                            else:
                                col_refs[q][j, rows, :] += sums[j]
                return carry

            zero = [jnp.zeros((8, 128), F32)] * tiles
            done = lax.fori_loop(0, 512 // STEP, step, [zero] * (4 if to_u else 1))
            for t in range(tiles):
                far = jnp.maximum(far, done[0][t])
            if to_u:
                done = done[1:]
                lanes[g] = [[a + b for a, b in zip(v, w)] for v, w in zip(lanes[g], done)] if g in lanes else done
    rows = {
        g: [
            jnp.concatenate([jnp.sum(v, axis=0, keepdims=True) for v in kind], axis=1) for kind in value
        ]
        for g, value in lanes.items()
    }
    return rows, far


def rows_of(part, sizes):
    return sum(sizes[i[2] if isinstance(i, tuple) else i] for i in part)


def scratch_for(q_parts, groups, sizes, width):
    q_bufs = [pltpu.VMEM((512 * len(q_parts), width), BF16)]
    u_sizes = [rows_of(p, sizes) if p else 0 for p in groups]
    u_bufs = [pltpu.VMEM((n or 16, width), BF16) for n in u_sizes]
    n_copies = sum(len(p) for p in q_parts) + sum(len(p) for p in groups if p)
    most = max([n or 512 for n in u_sizes])
    return q_bufs + u_bufs + [
        pltpu.VMEM((512 * len(q_parts), most), F32),
        pltpu.VMEM((len(q_parts), 4, 512, 128), F32),
        pltpu.SemaphoreType.DMA((n_copies,)),
    ]


def cost_of(tasks, q_parts, groups, sizes, width):
    def rows(p):
        return rows_of(p or q_parts[0], sizes)

    flops = sum(2 * 512 * len(t[1]) * rows(groups[t[0]]) * width for t in tasks)
    moved = 2 * width * sum(sizes)
    return pl.CostEstimate(flops=flops, transcendentals=0, bytes_accessed=moved)


VMEM_SPEC = pl.BlockSpec(memory_space=pltpu.VMEM)
SMEM_SPEC = pl.BlockSpec(memory_space=pltpu.SMEM)
ANY_SPEC = pl.BlockSpec(memory_space=pltpu.HBM)
LIMIT = pltpu.CompilerParams(vmem_limit_bytes=36 * 2**20)


def early_kernel(tasks, q_parts, groups, n_hbm, lane_outs, col_outs, side_ref_in, *refs):
    hbm, refs = refs[:n_hbm], refs[n_hbm:]
    n_notes = len(q_parts) + len(groups)
    notes, refs = refs[:n_notes], refs[n_notes:]
    lane_refs, refs = refs[: len(lane_outs)], refs[len(lane_outs) :]
    cols, refs = dict(zip(col_outs, refs)), refs[len(col_outs) :]
    far_ref, refs = refs[0], refs[1:]
    q_buf, refs = refs[0], refs[1:]
    u_bufs, (x_ref, side_ref, sems) = refs[: len(groups)], refs[len(groups) :]
    rows, far = pair_work(side_ref_in[0], tasks, q_parts, groups, hbm, notes, cols, q_buf, u_bufs, x_ref, side_ref, sems)
    for g, ref in zip(lane_outs, lane_refs):
        ref[...] = jnp.zeros_like(ref)
        for j in range(3):
            ref[j : j + 1, :] = rows[g][j]
    far_ref[...] = far


def early_pairs(edge, hbm, q_parts, groups, notes, tasks):
    sizes, width = [h.shape[0] for h in hbm], hbm[0].shape[1]
    lane_outs = [t[0] for t in tasks if any(v[1] for v in t[1])]
    col_outs = [q for q in range(len(q_parts)) if any(v[0] == q and v[2] for t in tasks for v in t[1])]
    shapes = [jax.ShapeDtypeStruct((8, notes[len(q_parts) + g].shape[1]), F32) for g in lane_outs]
    shapes += [jax.ShapeDtypeStruct((3, 512, 128), F32) for _ in col_outs]
    shapes += [jax.ShapeDtypeStruct((8, 128), F32)]
    out = pl.pallas_call(
        functools.partial(early_kernel, tasks, q_parts, groups, len(hbm), lane_outs, col_outs),
        out_shape=shapes,
        in_specs=[SMEM_SPEC] + [ANY_SPEC] * len(hbm) + [VMEM_SPEC] * len(notes),
        out_specs=[VMEM_SPEC] * len(shapes),
        scratch_shapes=scratch_for(q_parts, groups, sizes, width),
        cost_estimate=cost_of(tasks, q_parts, groups, sizes, width),
        compiler_params=LIMIT,
    )(edge.reshape(1), *hbm, *notes)
    n = len(lane_outs)
    return dict(zip(lane_outs, out)), dict(zip(col_outs, out[n:])), out[-1]


def last_kernel(tasks, q_parts, groups, n_hbm, lane_rows, n_cols, n_far, own_rows, side_ref_in, *refs):
    hbm, refs = refs[:n_hbm], refs[n_hbm:]
    n_notes = len(q_parts) + len(groups)
    notes, refs = refs[:n_notes], refs[n_notes:]
    lane_refs, refs = refs[: len(lane_rows)], refs[len(lane_rows) :]
    col_refs, refs = refs[: sum(n_cols)], refs[sum(n_cols) :]
    far_refs, refs = refs[:n_far], refs[n_far:]
    extra_ref, out_ref, refs = refs[0], refs[1], refs[2:]
    q_buf, refs = refs[0], refs[1:]
    u_bufs, refs = refs[: len(groups)], refs[len(groups) :]
    x_ref, side_ref, sems, col0_ref, col1_ref, g_ref = refs
    cols = {0: col0_ref, 1: col1_ref}
    rows, far = pair_work(side_ref_in[0], tasks, q_parts, groups, hbm, notes, cols, q_buf, u_bufs, x_ref, side_ref, sems)
    g_ref[...] = extra_ref[...]
    for ref, places in zip(lane_refs, lane_rows):
        for row, at, lo, m in places:
            g_ref[row : row + 3, at : at + m] += ref[0:3, lo : lo + m]
    for g, (row, at) in own_rows.items():
        for j in range(3):
            value = rows[g][j]
            g_ref[row + j : row + j + 1, at : at + value.shape[1]] += value
    start = 0
    for q, (n, row) in enumerate(zip(n_cols, (0, 8))):
        for j in range(3):
            total = cols[q][j]
            for ref in col_refs[start : start + n]:
                total = total + ref[j]
            across = jnp.sum(jnp.transpose(total), axis=0, keepdims=True)
            g_ref[row + j : row + j + 1, :] += across
        start += n
    for ref in far_refs:
        far = jnp.maximum(far, ref[...])
    far = jnp.max(jnp.max(far, axis=0, keepdims=True), axis=1, keepdims=True)
    g_ref[7:8, :] = jnp.broadcast_to(far, (1, 512))
    lane = iota((512, 512), 0)
    to_lane = (lane // 4 % 8) * 64 + (lane // 32) * 4 + lane % 4
    by_member = (to_lane == iota((512, 512), 1)).astype(BF16)
    parts = jnp.concatenate([p.astype(F32) for p in split3(g_ref[...])], axis=0).astype(BF16)
    given = jnp.dot(parts, by_member, preferred_element_type=F32)
    given = given[0:16] + given[16:32] + given[32:48]
    for m in range(8):
        piece = given[:, m * 64 : m * 64 + 64]
        page = jnp.concatenate([piece[0:8], piece[8:16]], axis=1)
        for copy in range(4):
            out_ref[m * 4 + copy] = page


def last_pairs(edge, hbm, q_parts, groups, notes, tasks, lanes, lane_rows, cols, fars, own_rows, extra):
    sizes, width = [h.shape[0] for h in hbm], hbm[0].shape[1]
    n_cols = tuple(len(c) for c in cols)
    small = lanes + [c for each in cols for c in each] + fars + [extra]
    return pl.pallas_call(
        functools.partial(
            last_kernel, tasks, q_parts, groups, len(hbm), lane_rows, n_cols, len(fars), own_rows
        ),
        out_shape=jax.ShapeDtypeStruct((32, 8, 128), F32),
        in_specs=[SMEM_SPEC] + [ANY_SPEC] * len(hbm) + [VMEM_SPEC] * (len(notes) + len(small)),
        out_specs=VMEM_SPEC,
        scratch_shapes=scratch_for(q_parts, groups, sizes, width)
        + [pltpu.VMEM((3, 512, 128), F32), pltpu.VMEM((3, 512, 128), F32), pltpu.VMEM((16, 512), F32)],
        cost_estimate=cost_of(tasks, q_parts, groups, sizes, width),
        compiler_params=LIMIT,
    )(edge.reshape(1), *hbm, *notes, *small)


def prep_kernel(pieces, own_ref, hit_ref, found_ref, half_ref, *refs):
    piece_refs, (buf, part, sems) = refs[: len(pieces)], refs[len(pieces) :]
    slab = 128
    n = buf.shape[0] // slab
    copies = [
        pltpu.make_async_copy(own_ref.at[i * slab : i * slab + slab, :], buf.at[i * slab : i * slab + slab, :], sems.at[i])
        for i in range(n)
    ]
    for copy in copies:
        copy.start()
    out = [
        pltpu.make_async_copy(buf.at[lo:hi, :], ref, sems.at[n + i])
        for i, ((lo, hi), ref) in enumerate(zip(pieces, piece_refs))
    ]
    for i, copy in enumerate(copies):
        copy.wait()
        for each, (lo, hi) in zip(out, pieces):
            if i * slab < hi <= i * slab + slab:
                each.start()

        def step(k, _, i=i):
            rows = pl.ds(pl.multiple_of(i * slab + k * 16, 16), 16)
            total = None
            for t in range(buf.shape[1] // 128):
                v = buf[rows, t * 128 : t * 128 + 128].astype(F32)
                total = v * v if total is None else total + v * v
            part[rows, :] = total
            return 0

        lax.fori_loop(0, slab // 16, step, 0)
    half_ref[...] = 0.5 * jnp.sum(jnp.transpose(part[...]), axis=0, keepdims=True)
    found = jnp.dot(hit_ref[...], buf[...], preferred_element_type=F32).astype(BF16)
    for i in range(8):
        found_ref[i] = found
    for each in out:
        each.wait()


def prepare(own, hit, pieces):
    width = own.shape[1]
    return pl.pallas_call(
        functools.partial(prep_kernel, pieces),
        out_shape=[jax.ShapeDtypeStruct((8, 8, width), BF16), jax.ShapeDtypeStruct((1, 512), F32)]
        + [jax.ShapeDtypeStruct((hi - lo, width), BF16) for lo, hi in pieces],
        in_specs=[ANY_SPEC, VMEM_SPEC],
        out_specs=[VMEM_SPEC] * 3 + [ANY_SPEC] * (len(pieces) - 1),
        scratch_shapes=[
            pltpu.VMEM((512, width), BF16),
            pltpu.VMEM((512, 128), F32),
            pltpu.SemaphoreType.DMA((4 + len(pieces),)),
        ],
        cost_estimate=pl.CostEstimate(flops=2 * 512 * 512 * width, transcendentals=0, bytes_accessed=own.size * 2),
        compiler_params=LIMIT,
    )(own, hit)


def close_kernel(width, where_ref, in_ref, order_ref, keep_ref, total_ref, gain_ref, cover_ref):
    lane = iota((4, 128), 1)
    row = iota((4, 128), 0)

    def page(line, sd):
        return in_ref[where_ref[0] + where_ref[1] * (line % 4) + sd]

    final = jnp.zeros((8, 512), F32)
    far = jnp.zeros((1, 64), F32)
    half_sum = jnp.zeros((1, 64), F32)
    for line in range(4):
        for sd in range(2):
            here = page(line, sd)
            far = jnp.maximum(far, here[7:8, 0:64])
            half_sum = half_sum + here[3:4, 64:128]
            low = here[0:4] + jnp.where(row < 3, page(line + 1, sd)[4:8], 0.0)
            fourth = page(line, 0) if sd == 1 else page(line + 1, 1)
            high = jnp.where(row < 3, page(line + 3, sd)[0:4] + fourth[4:8], 0.0)
            both = jnp.where(lane < 64, low, high)
            both = both[:, 0:64] + both[:, 64:128]
            both = jnp.concatenate([both, jnp.zeros((4, 64), F32)], axis=0)
            at = (line * 2 + sd) * 64
            parts = jnp.concatenate([p.astype(F32) for p in split3(both)], axis=0).astype(BF16)
            moved = jnp.dot(parts, order_ref[at : at + 64, :], preferred_element_type=F32)
            final = final + (moved[0:8] + moved[8:16] + moved[16:24])
    far = 2.0 * far[:, 0:1]
    half_sum = half_sum[:, 0:1]
    keep = keep_ref[...]
    total = total_ref[:, 0:1]
    scale = 1.0 / width
    gain_ref[0] = (2.0 * final[0:1] + total * far - 2.0 * half_sum) * scale * keep / total
    gain_ref[1] = 2.0 * final[1:2] * scale * keep / total
    gain_ref[2] = 2.0 * final[2:3] * scale * keep / total
    cover_ref[...] = keep * (far - 2.0 * final[3:4]) * scale


def source_of(x, z, y, core, row):
    group, sub, member, slot = row // 64, row // 32 % 2, row // 4 % 8, row % 4
    i, w = group // 4, group % 4
    outer = (y == 0) | (y == 3)
    low = y < 2
    y0 = jnp.where(outer, 3 * i, 1 + i)
    y1 = jnp.where(low, 1 - i, 2 + i)
    sx = jnp.where(core == 0, x, w)
    sz = jnp.where(core == 0, w, z)
    sy = jnp.where(core == 0, y0, y1)
    return dix(sx, sy, sz, jnp.where(sub == 0, 0, 1)), member, slot


def body(sketches, labels, places, counts, chosen):
    rows_dev, width = sketches.shape
    dp, cls = lax.axis_index("dp"), lax.axis_index("cls")
    x, zh, zl, y, core = dp // 2, dp % 2, cls // 8, cls // 2 % 4, cls % 2
    z = zh * 2 + zl
    edge = y % 2
    first = core == 0

    packed = jnp.concatenate([counts[0], jnp.broadcast_to(chosen, (3, 128))], axis=0)
    packed = send(packed, INFO)
    host_counts = packed[:8].astype(F32)
    picks = packed[8:11, 0]

    k_core, k_y, k_zl = labels % 2, labels // 2 % 4, labels // 8
    group = jnp.where(
        k_core == 0,
        (k_y // 2) * 4 + (k_y % 2) * 2 + k_zl,
        ((k_y + 3) % 4 // 2) * 4 + k_zl * 2 + k_y % 2,
    )
    spot = group * 64 + core * 32 + places // 512 * 4 + places % 4
    mine = jnp.where(k_core == core, spot, -1)
    theirs = jnp.where(k_core == core, -1, spot)
    from_twin = send(sketches, SWAP)
    twin_spot = send(theirs, SWAP)
    slots = iota((2 * rows_dev, rows_dev), 0)
    table_own = (slots == mine[None, :]).astype(BF16)
    table_twin = (slots == twin_spot[None, :]).astype(BF16)
    outgoing = (
        jnp.dot(table_own, sketches, preferred_element_type=F32)
        + jnp.dot(table_twin, from_twin, preferred_element_type=F32)
    ).astype(BF16)
    own = lax.all_to_all(
        outgoing.reshape(8, 64, width), AX, 0, 0, axis_index_groups=regroup_groups(), tiled=True
    ).reshape(512, width)

    src, member, slot = source_of(x, z, y, core, iota((1, 512), 1))
    place = member * 512 + src * 4 + slot
    seen = jnp.sum(
        jnp.where(iota((128, 512), 0) == src, exact(host_counts.T, (iota((8, 512), 0) == member).astype(F32)), 0.0),
        axis=0,
    )
    valid = slot[0].astype(F32) < seen
    n_valid = jnp.sum(host_counts)
    hit = (place == jnp.concatenate([picks, -jnp.ones((5,), jnp.int32)])[:, None]).astype(BF16)
    found, half, *cuts = prepare(own, hit, ((0, 128), (128, 256), (256, 384), (384, 512)))
    half = half[0]

    l = [send(v, UP) for v in cuts]
    first_relay = jnp.where(edge == 0, l[0], cuts[0])
    r = send(own, DOWN)

    found = lax.all_to_all(found, AX, 0, 0, axis_index_groups=class_groups(), tiled=True)
    found, _ = lax.optimization_barrier((found, first_relay))
    found = jnp.sum(found.astype(F32), axis=0).astype(BF16)
    to_picks = inner(found, own)
    second, to_picks = lax.optimization_barrier((l[1], to_picks))
    relays = [first_relay] + [jnp.where(edge == 0, v, cut) for v, cut in zip([second, *l[2:]], cuts[1:])]
    f = [send(v, ACROSS) for v in relays]
    pick_half = 0.5 * jnp.sum(jnp.square(found.astype(F32)), axis=1)
    near = pick_half[:3, None] - to_picks[:3]
    near1 = near[0]
    near2 = jnp.minimum(near[0], near[1])
    near3 = jnp.minimum(near2, near[2])
    info = jnp.stack(
        [half, jnp.where(valid, half, -BIG), jnp.where(valid, near1, -BIG), jnp.where(valid, near2, -BIG)]
        + [jnp.zeros((512,), F32)] * 4
    )
    info_l = send(info, UP)
    info_r = send(info, DOWN)
    info_f = send(info, FOURTH)

    mid = 256
    l_low, l_high = info_l[:, :mid], info_l[:, mid:]
    f_low, f_high = info_f[:, :mid], info_f[:, mid:]
    lanes_1, _, far_1 = early_pairs(edge, [own], [[0]], [None], [info, info], [(0, [(0, True, False)])])
    low = jnp.concatenate([l_low, f_low], axis=1)
    lanes_2, cols_2, far_2 = early_pairs(
        edge, [own, l[0], l[1], f[0], f[1]], [[0]], [[1, 2, 3, 4]], [info, low], [(0, [(0, True, True)])]
    )
    lanes_3, cols_3, far_3 = early_pairs(
        edge,
        [own, r, *l, f[0], f[1]],
        [[0], [1]],
        [[2, 3, 6, 7], [4, 5]],
        [info, info_r, low, l_high],
        [(0, [(1, True, True)]), (1, [(0, True, True), (1, False, True)])],
    )
    none = jnp.zeros((512,), F32)
    extra = [none] * 16
    extra[0] = -n_valid * half
    extra[3] = half + near3
    extra[11] = jnp.broadcast_to(jnp.sum(half), (512,))
    extra = jnp.stack(extra)
    lane_list = [
        (lanes_1[0], [(0, 0, 0, 512)]),
        (lanes_2[0], [(4, 0, 0, mid), (12, 0, mid, mid)]),
        (lanes_3[0], [(12, 0, mid, mid)]),
        (lanes_3[1], [(4, mid, 0, mid)]),
    ]
    outbox = last_pairs(
        edge,
        [own, r, f[2], f[3]],
        [[0], [1]],
        [[2, 3]],
        [info, info_r, f_high],
        [(0, [(0, True, True), (1, True, True)])],
        [v for v, _ in lane_list],
        [at for _, at in lane_list],
        [[cols_2[0], cols_3[0]], [cols_3[1]]],
        [far_1, far_2, far_3],
        {0: (12, mid)},
        extra,
    )
    inbox = lax.all_to_all(outbox, AX, 0, 0, axis_index_groups=final_groups(), tiled=True)

    lane1 = iota((512, 1), 0)
    line, sd, rest = lane1 // 128, lane1 // 64 % 2, lane1 % 64
    pair_y0 = y // 2 * 2 + sd
    pair_low = (y == 1) | (y == 2)
    pair_y1 = jnp.where(pair_low, 2 - sd, 3 * sd)
    pair_y = jnp.where(first, pair_y0, pair_y1)
    src2, _, slot2 = source_of(line, line, pair_y, core, (rest // 4) * 32 + rest % 4)
    in_order = (src2 * 4 + slot2 == iota((512, 512), 1)).astype(BF16)

    class_counts = counts[0]
    own_counts = lax.dynamic_index_in_dim(class_counts, dp, 0, keepdims=False)
    keep = (iota((128, 4), 1) < own_counts[:, None]).reshape(1, 512).astype(F32)
    total = jnp.broadcast_to(jnp.sum(class_counts).astype(F32), (1, 128))
    host = jnp.where(first, (edge * 2 + zl) * 2, (zl * 2 + edge) * 8)
    where = jnp.stack([host, jnp.where(first, 8, 2)])
    gains, cover = pl.pallas_call(
        functools.partial(close_kernel, width),
        out_shape=[jax.ShapeDtypeStruct((3, 1, 512), F32), jax.ShapeDtypeStruct((1, 512), F32)],
        in_specs=[pl.BlockSpec(memory_space=pltpu.SMEM)] + [VMEM_SPEC] * 4,
        out_specs=[VMEM_SPEC, VMEM_SPEC],
    )(where, inbox, in_order, keep, total)
    return (gains, cover)


def solution(mesh):
    placed = (
        P(("dp", "cls"), None),
        P(("dp", "cls")),
        P(("dp", "cls")),
        P("cls", None, None),
        P(None, "cls"),
    )
    return jax.shard_map(
        body,
        mesh=mesh,
        in_specs=placed,
        out_specs=(P(None, "cls", "dp"), P("cls", "dp")),
        check_vma=False,
    )
```
